256 devices in a mesh: gz: 64 (over x, z_hi, y), xy: 4 (over z_lo, core).
Axes of the slice: x: 4, y: 4, z: 8 (z_hi: 4, z_lo: 2; z = z_hi * 2 + z_lo), core: 2. Of those that a mesh axis runs over, the one named last changes fastest.
Arguments:
- patches: bfloat16 [64, 8, 16, 128, 128], P('gz', 'xy'), may hold values from -6 to 6
- peak_offsets: int32 [64, 6, 8, 16], P('gz', None, 'xy'), may hold values from -4 to 4
- valid_masks: int32 [64, 3, 8, 16], P('gz', None, 'xy'), may hold values 0 or 1
- initial_positions: float32 [2, 64, 128, 256], P(None, 'gz', 'xy'), may hold values from -40 to 40
Outputs:
- positions: float32 [2, 64, 128, 256], P(None, 'gz', 'xy')
- targets: float32 [64, 6, 8, 16], P('gz', None, 'xy')
- surfaces: bfloat16 [64, 3, 8, 16, 128, 128], P('gz', None, 'xy')
- force_rms: float32 [4], replicated
The draws below stay inside these ranges and needn't reach their ends.
All inputs are finite; a program needn't handle non-finite values. No bound on the sum of `valid_masks` on one device may be relied on, other than what follows from the above.
Results may differ from the reference program's by a relative error of at most 0.0091.
Values may be sent and summed in bfloat16 or wider, within the bound.
A program may use at most 64 MiB of HBM per device.

```python
import math
import jax
import jax.numpy as jnp
from jax import lax

S = 128
SUB = 16
GC = 16
ITERS = 4
NZ = 64
GR = 8
NROWS = 128
NCOLS = 256


def draw_initial_positions(key, part):
    first_key = jax.random.fold_in(key, 0)
    third_key = jax.random.fold_in(key, 2)
    fourth_key = jax.random.fold_in(key, 3)
    depth_series = jnp.arange(NZ, dtype=jnp.float32)
    growth = 1.0 + 2.0 * depth_series / max(NZ - 1, 1)
    roughness = jax.random.uniform(third_key, (NZ,), jnp.float32, 0.75, 1.25)
    jitter = jax.random.uniform(fourth_key, (NROWS,), jnp.float32, 0.0, 1.0)
    level = (jnp.arange(NROWS, dtype=jnp.float32) + jitter) / NROWS
    base = jax.random.normal(first_key, (2, NZ, NROWS, NCOLS), jnp.float32)
    base = jnp.clip(base, -3.3, 3.3)
    row_scale = 0.3 * jnp.power(10.0, level)
    depth_scale = growth * roughness
    return base * depth_scale[None, :, None, None] * row_scale[None, None, :, None]


def plant(result, key, smallest, top_value):
    dims = result.shape
    spot = [jax.random.randint(jax.random.fold_in(key, axis), (), 0, dims[axis]) for axis in range(len(dims))]
    result = result.at[tuple(spot)].set(smallest)
    longest = dims.index(max(dims))
    spot[longest] = (spot[longest] + 1) % dims[longest]
    return result.at[tuple(spot)].set(top_value)


def steps_of(stream_key, shape, cuts, low, top_value):
    gain, own = 1.0, jax.random.fold_in(stream_key, 6)
    for position, blocks in cuts:
        steps = jnp.exp(jax.random.uniform(jax.random.fold_in(own, position), (blocks,), jnp.float32, low / len(cuts), top_value / len(cuts)))
        gain = gain * jnp.repeat(steps, shape[position] // blocks).reshape([-1 if axis == position else 1 for axis in range(len(shape))])
    return gain


def noise(key, extent, deviation, limit, pieces=(), held_as=jnp.bfloat16):
    values = deviation * jax.random.normal(key, extent, jnp.float32)
    if pieces:
        values = values * steps_of(key, extent, pieces, -0.22, 0.18)
    return jnp.clip(values, -limit, limit).astype(held_as)


def setup_inputs(seed: int = 0) -> dict:
    arg_keys = jax.random.split(jax.random.key(seed), 5)
    patches = noise(arg_keys[0], (NZ, GR, GC, S, S), 1.0, 6.0, ((0, 64), (1, 4)))
    peak_offsets = plant(jax.random.randint(arg_keys[1], (NZ, 6, GR, GC), -4, 5), jax.random.fold_in(arg_keys[1], 1), -4, 4).astype(jnp.int32)
    valid_masks = plant((jax.random.randint(arg_keys[2], (NZ, 3, GR, GC), 0, 4) < 3).astype(jnp.int32), jax.random.fold_in(arg_keys[2], 1), 0, 1)
    initial_positions = draw_initial_positions(jax.random.fold_in(arg_keys[4], 71), 0)
    return {"patches": patches, "peak_offsets": peak_offsets, "valid_masks": valid_masks, "initial_positions": initial_positions}


lattice_stiff = 0.5
clip_level = 5.0
step_size = 0.2
floor_ratio = 0.4
tiny_eps = 1e-06

def dft_tables(length):
    series = jnp.arange(length, dtype=jnp.int32)
    product = series[:, None] * series[None, :] % length
    angles = 2.0 * math.pi / length * product.astype(jnp.float32)
    return (jnp.cos(angles).astype(jnp.bfloat16), jnp.sin(angles).astype(jnp.bfloat16))

def rounded(value):
    return lax.optimization_barrier(value.astype(jnp.bfloat16)).astype(jnp.float32)

def spectrum(tiles, cosine, sine):
    row_cos = rounded(jnp.einsum('pab,bk->pak', tiles, cosine))
    row_sin = rounded(jnp.einsum('pab,bk->pak', tiles, sine))
    real = jnp.einsum('ja,pak->pjk', cosine, row_cos) - jnp.einsum('ja,pak->pjk', sine, row_sin)
    imag = -(jnp.einsum('ja,pak->pjk', sine, row_cos) + jnp.einsum('ja,pak->pjk', cosine, row_sin))
    return (real, imag)

def correlate(first, second, cosine, sine, length):
    cross_real = rounded(first[0] * second[0] + first[1] * second[1])
    cross_imag = rounded(first[0] * second[1] - first[1] * second[0])
    half_real = rounded(jnp.einsum('pab,bk->pak', cross_real, cosine) - jnp.einsum('pab,bk->pak', cross_imag, sine))
    half_imag = rounded(jnp.einsum('pab,bk->pak', cross_real, sine) + jnp.einsum('pab,bk->pak', cross_imag, cosine))
    whole = jnp.einsum('ja,pak->pjk', cosine, half_real) - jnp.einsum('ja,pak->pjk', sine, half_imag)
    return whole / float(length * length)

def refine(corr, shift_rows, shift_cols, length):
    series = jnp.arange(length, dtype=jnp.int32)
    taps = jnp.arange(3, dtype=jnp.int32) - 1
    row_index = (shift_rows[:, None] + taps[None, :] + length) % length
    col_index = (shift_cols[:, None] + taps[None, :] + length) % length
    row_pick = (series[None, None, :] == row_index[:, :, None]).astype(jnp.float32)
    col_pick = (series[None, None, :] == col_index[:, :, None]).astype(jnp.float32)
    partial_rows = jnp.einsum('pta,pab->ptb', row_pick, corr, precision=lax.Precision.HIGHEST)
    values = jnp.einsum('ptb,psb->pts', partial_rows, col_pick, precision=lax.Precision.HIGHEST)
    floor_value = floor_ratio * length
    along_rows = values[:, :, 1]
    along_cols = values[:, 1, :]
    sub_rows = (along_rows[:, 2] - along_rows[:, 0]) / jnp.maximum(lax.optimization_barrier(jnp.sum(jnp.abs(along_rows), axis=1)), floor_value)
    sub_cols = (along_cols[:, 2] - along_cols[:, 0]) / jnp.maximum(lax.optimization_barrier(jnp.sum(jnp.abs(along_cols), axis=1)), floor_value)
    return (shift_rows.astype(jnp.float32) + sub_rows, shift_cols.astype(jnp.float32) + sub_cols)

def raise_depth(array, distance, axis):
    zeros = jnp.zeros_like(lax.slice_in_dim(array, 0, distance, axis=axis))
    joined = jnp.concatenate([array, zeros], axis=axis)
    return lax.slice_in_dim(joined, distance, distance + array.shape[axis], axis=axis)

def lower_depth(array, distance, axis):
    zeros = jnp.zeros_like(lax.slice_in_dim(array, 0, distance, axis=axis))
    joined = jnp.concatenate([zeros, array], axis=axis)
    return lax.slice_in_dim(joined, 0, array.shape[axis], axis=axis)

def expand_nodes(array, axis):
    return jnp.repeat(jnp.repeat(array, SUB, axis=axis), SUB, axis=axis + 1)

def reference(patches, peak_offsets, valid_masks, initial_positions):
    tiles_count = GR * GC
    cos_table, sin_table = dft_tables(S)
    cosine = cos_table.astype(jnp.float32)
    sine = sin_table.astype(jnp.float32)
    padded = jnp.concatenate([patches, jnp.zeros((3, GR, GC, S, S), jnp.bfloat16)], axis=0)

    def one_section(depth_index):
        window = lax.dynamic_slice_in_dim(padded, depth_index, 4, 0).astype(jnp.float32).reshape(4, tiles_count, S, S)
        own = spectrum(window[0], cosine, sine)
        offsets = lax.dynamic_index_in_dim(peak_offsets, depth_index, 0, keepdims=False).reshape(6, tiles_count)
        results = []
        maps = []
        for distance in range(3):
            other = spectrum(window[distance + 1], cosine, sine)
            corr = correlate(own, other, cosine, sine, S)
            maps.append(corr.astype(jnp.bfloat16).reshape(GR, GC, S, S))
            rows_target, cols_target = refine(corr, offsets[2 * distance], offsets[2 * distance + 1], S)
            results.append(rows_target)
            results.append(cols_target)
        return (jnp.stack(results).reshape(6, GR, GC), jnp.stack(maps))
    targets, surfaces = lax.map(one_section, jnp.arange(NZ, dtype=jnp.int32))
    depth_series = jnp.arange(NZ, dtype=jnp.int32)
    weights = []
    vectors = []
    for distance in range(1, 4):
        live = (depth_series + distance < NZ).astype(jnp.float32)
        patch_weight = valid_masks[:, distance - 1].astype(jnp.float32) * (1.0 / distance) * live[:, None, None]
        weights.append(expand_nodes(patch_weight, 1))
        patch_vector = jnp.stack([targets[:, 2 * distance - 2], targets[:, 2 * distance - 1]], axis=0)
        vectors.append(expand_nodes(patch_vector, 2))
    count = 2.0 * NZ * NROWS * NCOLS
    positions = initial_positions
    norms = []
    for iteration in range(ITERS):
        edged = jnp.pad(positions, ((0, 0), (0, 0), (1, 1), (1, 1)), mode='edge')
        lattice = edged[:, :, :-2, 1:-1] + edged[:, :, 2:, 1:-1] + edged[:, :, 1:-1, :-2] + edged[:, :, 1:-1, 2:] - 4.0 * positions
        force = lattice_stiff * lattice
        for distance in range(1, 4):
            weight = weights[distance - 1]
            vector = vectors[distance - 1]
            above = raise_depth(positions, distance, 1)
            below = lower_depth(positions, distance, 1)
            weight_low = lower_depth(weight, distance, 0)
            vector_low = lower_depth(vector, distance, 1)
            force = force + weight * (above - positions - vector) - weight_low * (positions - below - vector_low)
        rms = jnp.sqrt(jnp.sum(force * force) / count + tiny_eps)
        factor = jnp.minimum(1.0, clip_level / rms)
        positions = positions + step_size * factor * force
        norms.append(rms)
    return (positions, targets, surfaces, jnp.stack(norms))
```

```python
import functools

import numpy as np

import jax
import jax.numpy as jnp
from jax import lax
from jax.experimental import pallas as pl
from jax.experimental.pallas import tpu as pltpu
from jax.sharding import PartitionSpec as P

SUB = 16
ITERS = 4
LINE = 4
CHUNKS = 16

lattice_stiff = 0.5
clip_level = 5.0
step_size = 0.2
floor_ratio = 0.4
tiny_eps = 1e-06

MESH = pl.DeviceIdType.MESH
F32 = jnp.float32
BF16 = jnp.bfloat16
PAIRS = [(i, j) for i in range(ITERS) for j in range(i, ITERS)]


def tables(length):
    series = np.arange(length)
    angles = 2.0 * np.pi / length * (series[:, None] * series[None, :] % length)
    cosine = np.cos(angles).astype(jnp.bfloat16)
    sine = np.sin(angles).astype(jnp.bfloat16)
    right = np.concatenate([cosine, sine], axis=1)
    left = np.block([[cosine, -sine], [-sine, -cosine]])
    back = np.block([[cosine, sine], [-sine, cosine]])
    last = np.concatenate([cosine, -sine], axis=1)
    return right, left, back, last


def kernel(
    depth,
    tiles,
    patches,
    offsets,
    offsets_v,
    masks,
    start,
    right,
    left,
    back,
    last,
    positions,
    targets,
    surfaces,
    norms,
    own,
    near,
    cross,
    spec_real,
    spec_imag,
    staged,
    taps,
    send_z,
    recv_z,
    send_e,
    recv_e,
    weight_t,
    weight_l,
    target_t,
    target_l,
    weights,
    fields,
    gram,
    gram_a,
    gram_b,
    local_sem,
    surf_sem,
    ps,
    pr,
    zs,
    zr,
    es,
    er,
    ws,
    wr,
    ts,
    tr,
    gs,
    gr,
):
    z = lax.axis_index("gz")
    t = lax.axis_index("xy")
    count, length, _ = own.shape
    piece = count // CHUNKS
    columns = masks.shape[2]
    rows_dev = masks.shape[1]
    lines = depth // LINE
    y = lax.rem(z, LINE)
    line = lax.div(z, LINE)
    has_next = line < lines - 1
    has_prev = line > 0
    group = LINE * tiles
    me = y * tiles + t

    def remote(src, dst, send, recv, gz, xy):
        return pltpu.make_async_remote_copy(
            src_ref=src, dst_ref=dst, send_sem=send, recv_sem=recv, device_id=(gz, xy), device_id_type=MESH
        )

    def local_copy(c):
        part = pl.ds(c * piece, piece)
        return pltpu.make_async_copy(patches.at[part], own.at[part], local_sem.at[c])

    def start_local(c, carry):
        local_copy(c).start()
        return carry

    lax.fori_loop(0, CHUNKS, start_local, 0)

    barrier = pltpu.get_barrier_semaphore()

    def greet_group(i, carry):
        other = lax.rem(me + i, group)
        gz = line * LINE + lax.div(other, tiles)
        pl.semaphore_signal(barrier, inc=1, device_id=(gz, lax.rem(other, tiles)), device_id_type=MESH)
        return carry

    lax.fori_loop(1, group, greet_group, 0)

    def greet_lines(i, carry):
        other = lax.rem(line + i, lines)
        pl.semaphore_signal(barrier, inc=1, device_id=(other * LINE + y, t), device_id_type=MESH)
        return carry

    lax.fori_loop(1, lines, greet_lines, 0)
    for k in range(1, 4):
        for sign in (-1, 1):
            there = z + sign * k

            @pl.when((there >= 0) & (there < depth))
            def _():
                pl.semaphore_signal(barrier, inc=1, device_id=(there, t), device_id_type=MESH)

    for k in range(1, 4):

        @pl.when(z + k >= depth)
        def _():
            near[k - 1] = jnp.zeros(near.shape[1:], BF16)
            for r in range(ITERS):
                recv_z[r, k - 1] = jnp.zeros(recv_z.shape[2:], BF16)

        @pl.when(z - k < 0)
        def _():
            for r in range(ITERS):
                recv_z[r, 2 + k] = jnp.zeros(recv_z.shape[2:], BF16)
            weight_l[k - 1] = jnp.zeros(weight_l.shape[1:], F32)
            target_l[k - 1] = jnp.zeros(target_l.shape[1:], F32)

    weight_t[...] = jnp.zeros(weight_t.shape, F32)
    target_t[...] = jnp.zeros(target_t.shape, F32)
    taps[...] = jnp.zeros(taps.shape, F32)
    for k in range(1, 4):
        live = jnp.where(z + k < depth, 1.0 / k, 0.0).astype(F32)
        weight_t[2 * (k - 1) : 2 * k, 0:columns] = masks[k - 1].astype(F32) * live

    def stage(r, value):
        for a in range(2):
            send_z[r, a] = value[a].astype(BF16)
            send_e[r, 0, a : a + 1] = value[a][0:1]
            send_e[r, 1, a : a + 1] = value[a][-1:]

    start_value = [start[0], start[1]]
    stage(0, start_value)

    expected = group - 1 + lines - 1
    for k in range(1, 4):
        expected = expected + (z + k < depth).astype(jnp.int32) + (z - k >= 0).astype(jnp.int32)
    pl.semaphore_wait(barrier, expected)

    def z_copy(r, k, sign):
        slot = 2 + k if sign > 0 else k - 1
        return remote(send_z.at[r], recv_z.at[r, slot], zs.at[r, slot], zr.at[r, slot], z + sign * k, t)

    def e_copy(r, sign):
        side = 1 if sign > 0 else 0
        return remote(send_e.at[r, side], recv_e.at[r, 1 - side], es.at[r, side], er.at[r, 1 - side], z, t + sign)

    def exchange_start(r):
        for k in (3, 2, 1):
            for sign in (-1, 1):

                @pl.when((z + sign * k >= 0) & (z + sign * k < depth))
                def _():
                    z_copy(r, k, sign).start()

        for sign in (-1, 1):

            @pl.when((t + sign >= 0) & (t + sign < tiles))
            def _():
                e_copy(r, sign).start()

    def exchange_wait(r):
        for k in (1, 2, 3):
            for sign in (-1, 1):

                @pl.when((z - sign * k >= 0) & (z - sign * k < depth))
                def _():
                    z_copy(r, k, sign).wait_recv()

        for sign in (-1, 1):

            @pl.when((t - sign >= 0) & (t - sign < tiles))
            def _():
                e_copy(r, sign).wait_recv()

    def exchange_drain(r):
        for k in (1, 2, 3):
            for sign in (-1, 1):

                @pl.when((z + sign * k >= 0) & (z + sign * k < depth))
                def _():
                    z_copy(r, k, sign).wait_send()

        for sign in (-1, 1):

            @pl.when((t + sign >= 0) & (t + sign < tiles))
            def _():
                e_copy(r, sign).wait_send()

    def w_copy(k):
        return remote(weight_t, weight_l.at[k - 1], ws.at[k - 1], wr.at[k - 1], z + k, t)

    def t_copy(k):
        return remote(target_t.at[k - 1], target_l.at[k - 1], ts.at[k - 1], tr.at[k - 1], z + k, t)

    def part_of(c):
        return pl.ds(c * piece, piece)

    def patch_copy(src, dst, send, slot, c, gz):
        part = part_of(c)
        return remote(src.at[part], dst.at[part], ps.at[send], pr.at[slot, c], gz, t)

    own_sends = [
        ((y < LINE - 1) & has_prev, own, cross, 0, 3, z - LINE),
        (y >= 1, own, near.at[0], 1, 0, z - 1),
        (y == LINE - 1, own, near.at[2], 2, 2, z - 3),
    ]
    cross_sends = [
        ((y < LINE - 1) & has_next, cross, near.at[2], 3, 2, z + 1),
        ((y == 0) & has_next, cross, near.at[0], 4, 0, z + 3),
    ]
    first_sends = [((y == 1) | (y == 2), near.at[0], near.at[1], 5, 1, z - 1)]
    third_sends = [(((y == 1) | (y == 2)) & has_next, near.at[2], near.at[1], 6, 1, z + 1)]
    all_sends = own_sends + cross_sends + first_sends + third_sends

    def send_all(sends, c):
        for condition, src, dst, send, slot, gz in sends:

            @pl.when(condition)
            def _():
                patch_copy(src, dst, send, slot, c, gz).start()

    def arrived(slot, c):
        buffer = cross if slot == 3 else near.at[slot]
        patch_copy(buffer, buffer, 0, slot, c, z).wait_recv()

    exchange_start(0)
    for k in range(1, 4):

        @pl.when(z + k < depth)
        def _():
            w_copy(k).start()

    def send_own(c, carry):
        local_copy(c).wait()
        send_all(own_sends, c)
        return carry

    lax.fori_loop(0, CHUNKS, send_own, 0)

    half = length

    def dot(a, b):
        return jnp.dot(a, b, preferred_element_type=F32)

    def side_by_side(m):
        return jnp.concatenate(
            [
                jnp.concatenate([m[:half, :half], m[half:, :half]], axis=1),
                jnp.concatenate([m[:half, half:], m[half:, half:]], axis=1),
            ],
            axis=0,
        )

    def spectra(ref, p):
        pair = ref[pl.ds(p, 2)].reshape(2 * half, half)
        mixed = dot(pair, right[...]).astype(BF16)
        return dot(left[...], side_by_side(mixed))

    def own_spectra(c):
        def body(i, carry):
            p = c * piece + 2 * i
            s = spectra(own, p)
            for a in range(2):
                cols = slice(a * half, (a + 1) * half)
                spec_real[p + a] = s[:half, cols]
                spec_imag[p + a] = s[half:, cols]
            return carry

        lax.fori_loop(0, piece // 2, body, 0)

    row_id = lax.broadcasted_iota(jnp.int32, (16, length), 0)
    row_id = jnp.where(row_id < 8, row_id, row_id - 16)
    col_id = lax.broadcasted_iota(jnp.int32, (16, length), 1)
    col_id = jnp.where(col_id < length // 2, col_id, col_id - length)
    tap_row = lax.broadcasted_iota(jnp.int32, (8, length), 0)
    tap_col = lax.broadcasted_iota(jnp.int32, (8, length), 1)

    def pick(k, p, window):
        r = lax.div(p, columns)
        c = lax.rem(p, columns)
        d_row = row_id - offsets[2 * k, r, c]
        d_col = col_id - offsets[2 * k + 1, r, c]
        down = jnp.where((d_col == 0) & (jnp.abs(d_row) <= 1), window, 0.0)
        across = jnp.where((d_row == 0) & (jnp.abs(d_col) <= 1), window, 0.0)

        def total(v):
            return jnp.sum(jnp.sum(v, axis=0, keepdims=True), axis=1, keepdims=True)

        sums = (
            total(down * d_row.astype(F32)),
            total(jnp.abs(down)),
            total(across * d_col.astype(F32)),
            total(jnp.abs(across)),
        )
        value = taps[k]
        for q in range(4):
            value = jnp.where((tap_row == 2 * q + r) & (tap_col == c), sums[q], value)
        taps[k] = value

    def correlate(k, c):
        def body(i, carry):
            p = c * piece + 2 * i
            s = spectra(near.at[k], p)
            mixed = []
            for a in range(2):
                cols = slice(a * half, (a + 1) * half)
                b_real, b_imag = s[:half, cols], s[half:, cols]
                a_real, a_imag = spec_real[p + a], spec_imag[p + a]
                real = (a_real * b_real + a_imag * b_imag).astype(BF16)
                imag = (a_real * b_imag - a_imag * b_real).astype(BF16)
                mixed.append(jnp.concatenate([real, imag], axis=1))
            halves = dot(jnp.concatenate(mixed, axis=0), back[...]).astype(BF16)
            corr = dot(last[...], side_by_side(halves)) * (1.0 / (length * length))
            for a in range(2):
                one = corr[:, a * half : (a + 1) * half]
                staged[k, p + a] = one.astype(BF16)
                pick(k, p + a, jnp.concatenate([one[:8], one[length - 8 :]], axis=0))
            return carry

        lax.fori_loop(0, piece // 2, body, 0)
        part = part_of(c)
        pltpu.make_async_copy(staged.at[k, part], surfaces.at[k, part], surf_sem).start()

    def step(c, carry):
        @pl.when(c < CHUNKS)
        def _():
            own_spectra(c)

            @pl.when(z + 1 < depth)
            def _():
                arrived(0, c)

            send_all(first_sends, c)

            @pl.when((y < LINE - 1) & has_next)
            def _():
                arrived(3, c)

            send_all(cross_sends, c)
            correlate(0, c)

        @pl.when((c >= 1) & (c < CHUNKS + 1))
        def _():
            @pl.when(z + 3 < depth)
            def _():
                arrived(2, c - 1)

            send_all(third_sends, c - 1)
            correlate(2, c - 1)

        @pl.when(c >= 2)
        def _():
            @pl.when(z + 2 < depth)
            def _():
                arrived(1, c - 2)

            correlate(1, c - 2)

        return carry

    lax.fori_loop(0, CHUNKS + 2, step, 0)

    for k in range(1, 4):
        sums = taps[k - 1]
        weight = weight_t[2 * (k - 1) : 2 * k, 0:columns]
        for a in range(2):
            slope = sums[4 * a : 4 * a + 2, 0:columns]
            size = sums[4 * a + 2 : 4 * a + 4, 0:columns]
            shift = offsets_v[2 * (k - 1) + a].astype(F32)
            value = shift + slope / jnp.maximum(size, floor_ratio * length)
            targets[2 * (k - 1) + a] = value
            target_t[k - 1, 2 * a : 2 * a + 2, 0:columns] = weight * value
    for k in range(1, 4):

        @pl.when(z + k < depth)
        def _():
            t_copy(k).start()

    nodes_rows, nodes_cols = start.shape[1], start.shape[2]
    spread = (
        lax.broadcasted_iota(jnp.int32, (length, nodes_cols), 0)
        == lax.shift_right_logical(lax.broadcasted_iota(jnp.int32, (length, nodes_cols), 1), 4)
    ).astype(F32)

    def widen(small):
        return jnp.dot(small, spread, precision=lax.Precision.HIGHEST, preferred_element_type=F32)

    def tall(wide, first):
        return jnp.concatenate(
            [jnp.broadcast_to(wide[first + r : first + r + 1], (SUB, nodes_cols)) for r in range(rows_dev)], axis=0
        )

    wide_own = widen(weight_t[...])
    for k in range(1, 4):

        @pl.when(z - k >= 0)
        def _():
            w_copy(k).wait_recv()

        weights[k - 1] = tall(wide_own, 2 * (k - 1))
        weights[2 + k] = tall(widen(weight_l[k - 1]), 2 * (k - 1))

    node_row = lax.broadcasted_iota(jnp.int32, (nodes_rows, nodes_cols), 0)
    node_col = lax.broadcasted_iota(jnp.int32, (nodes_rows, nodes_cols), 1)

    def linear(r, value):
        result = []
        for a in range(2):
            u = value[a]
            upper = jnp.where(t == 0, u[0:1], recv_e[r, 0, a : a + 1])
            lower = jnp.where(t == tiles - 1, u[-1:], recv_e[r, 1, a : a + 1])
            up = jnp.where(node_row == 0, upper, pltpu.roll(u, 1, 0))
            down = jnp.where(node_row == nodes_rows - 1, lower, pltpu.roll(u, nodes_rows - 1, 0))
            west = jnp.where(node_col == 0, u, pltpu.roll(u, 1, 1))
            east = jnp.where(node_col == nodes_cols - 1, u, pltpu.roll(u, nodes_cols - 1, 1))
            force = lattice_stiff * (up + down + west + east - 4.0 * u)
            for k in range(1, 4):
                force = force + weights[k - 1] * (recv_z[r, k - 1, a].astype(F32) - u)
                force = force - weights[2 + k] * (u - recv_z[r, 2 + k, a].astype(F32))
            result.append(force)
        return result

    exchange_wait(0)
    base = linear(0, start_value)

    for k in range(1, 4):

        @pl.when(z - k >= 0)
        def _():
            t_copy(k).wait_recv()

    pull = target_l[0] + target_l[1] + target_l[2] - target_t[0] - target_t[1] - target_t[2]
    wide_pull = widen(pull)
    value = [base[a] + tall(wide_pull, 2 * a) for a in range(2)]
    for i in range(ITERS):
        for a in range(2):
            fields[i, a] = value[a]
        if i < ITERS - 1:
            stage(i + 1, value)
            exchange_start(i + 1)
        for n, (first, second) in enumerate(PAIRS):
            if second == i:
                product = fields[first, 0] * value[0] + fields[first, 1] * value[1]
                row = jnp.sum(product, axis=0, keepdims=True)
                gram[n : n + 1] = row[:, :length] + row[:, length:]
        if i < ITERS - 1:
            exchange_wait(i + 1)
            moved = linear(i + 1, value)
            value = [value[a] + step_size * moved[a] for a in range(2)]

    def group_copy(i):
        other = lax.rem(me + i, group)
        return remote(
            gram, gram_a.at[me], gs.at[0, i], gr.at[0, i], line * LINE + lax.div(other, tiles), lax.rem(other, tiles)
        )

    def lines_copy(i):
        other = lax.rem(line + i, lines)
        return remote(gram, gram_b.at[line], gs.at[1, i], gr.at[1, i], other * LINE + y, t)

    def run(copy, number, what):
        def body(i, carry):
            getattr(copy(i), what)()
            return carry

        lax.fori_loop(1, number, body, 0)

    for n in range(len(PAIRS), gram.shape[0]):
        gram[n : n + 1] = jnp.zeros((1, length), F32)
    run(group_copy, group, "start")
    gram_a[me] = gram[...]
    run(group_copy, group, "wait")
    total = gram_a[0]
    for i in range(1, group):
        total = total + gram_a[i]
    gram[...] = total
    run(lines_copy, lines, "start")
    gram_b[line] = total
    run(lines_copy, lines, "wait")
    total = gram_b[0]
    for i in range(1, lines):
        total = total + gram_b[i]
    total = jnp.broadcast_to(jnp.sum(total, axis=1, keepdims=True), total.shape)

    entries = {}
    for n, (first, second) in enumerate(PAIRS):
        entries[first, second] = entries[second, first] = total[n : n + 1]
    number = 2.0 * depth * tiles * nodes_rows * nodes_cols
    ones = jnp.ones((1, length), F32)
    coefficients = [ones]
    sums = [jnp.zeros((1, length), F32)] * ITERS
    for i in range(ITERS):
        square = jnp.zeros((1, length), F32)
        for first in range(len(coefficients)):
            for second in range(len(coefficients)):
                square = square + coefficients[first] * coefficients[second] * entries[first, second]
        rms = jnp.sqrt(jnp.maximum(square, 0.0) / number + tiny_eps)
        norms[i : i + 1] = rms
        factor = jnp.minimum(1.0, clip_level / rms)
        for n in range(len(coefficients)):
            sums[n] = sums[n] + step_size * factor * coefficients[n]
        kept = [(1.0 - factor) * value for value in coefficients] + [0.0 * ones]
        shifted = [0.0 * ones] + [factor * value for value in coefficients]
        coefficients = [kept[n] + shifted[n] for n in range(len(shifted))]
    for a in range(2):
        result = start[a]
        for n in range(ITERS):
            result = result + jnp.concatenate([sums[n], sums[n]], axis=1) * fields[n, a]
        positions[a] = result

    for k in range(1, 4):

        @pl.when(z + k < depth)
        def _():
            w_copy(k).wait_send()
            t_copy(k).wait_send()

    for r in range(ITERS):
        exchange_drain(r)
    for condition, src, dst, send, slot, gz in all_sends:

        @pl.when(condition)
        def _():
            remote(src, dst, ps.at[send], pr.at[slot, 0], gz, t).wait_send()

    pltpu.make_async_copy(staged, surfaces, surf_sem).wait()


def local(depth, tiles, patches, peak_offsets, valid_masks, initial_positions):
    _, rows_dev, columns, length, _ = patches.shape
    count = rows_dev * columns
    _, _, nodes_rows, nodes_cols = initial_positions.shape
    offsets = peak_offsets.reshape(6, rows_dev, columns)
    vmem = pl.BlockSpec(memory_space=pltpu.VMEM)
    smem = pl.BlockSpec(memory_space=pltpu.SMEM)
    hbm = pl.BlockSpec(memory_space=pl.ANY)
    group = LINE * tiles
    lines = depth // LINE
    dma = pltpu.SemaphoreType.DMA
    flops = 2 * count * (4 * 6 + 3 * 6) * length**3
    outs = pl.pallas_call(
        functools.partial(kernel, depth, tiles),
        out_shape=(
            jax.ShapeDtypeStruct((2, nodes_rows, nodes_cols), F32),
            jax.ShapeDtypeStruct((6, rows_dev, columns), F32),
            jax.ShapeDtypeStruct((3, count, length, length), BF16),
            jax.ShapeDtypeStruct((ITERS, length), F32),
        ),
        in_specs=[hbm, smem, vmem, vmem, vmem, vmem, vmem, vmem, vmem],
        out_specs=(vmem, vmem, hbm, vmem),
        scratch_shapes=[
            pltpu.VMEM((count, length, length), BF16),
            pltpu.VMEM((3, count, length, length), BF16),
            pltpu.VMEM((count, length, length), BF16),
            pltpu.VMEM((count, length, length), F32),
            pltpu.VMEM((count, length, length), F32),
            pltpu.VMEM((3, count, length, length), BF16),
            pltpu.VMEM((3, 8, length), F32),
            pltpu.VMEM((ITERS, 2, nodes_rows, nodes_cols), BF16),
            pltpu.VMEM((ITERS, 6, 2, nodes_rows, nodes_cols), BF16),
            pltpu.VMEM((ITERS, 2, 8, nodes_cols), F32),
            pltpu.VMEM((ITERS, 2, 8, nodes_cols), F32),
            pltpu.VMEM((8, length), F32),
            pltpu.VMEM((3, 8, length), F32),
            pltpu.VMEM((3, 8, length), F32),
            pltpu.VMEM((3, 8, length), F32),
            pltpu.VMEM((6, nodes_rows, nodes_cols), F32),
            pltpu.VMEM((ITERS, 2, nodes_rows, nodes_cols), F32),
            pltpu.VMEM((16, length), F32),
            pltpu.VMEM((group, 16, length), F32),
            pltpu.VMEM((lines, 16, length), F32),
            dma((CHUNKS,)),
            dma,
            dma((7,)),
            dma((4, CHUNKS)),
            dma((ITERS, 6)),
            dma((ITERS, 6)),
            dma((ITERS, 2)),
            dma((ITERS, 2)),
            dma((3,)),
            dma((3,)),
            dma((3,)),
            dma((3,)),
            dma((2, max(group, lines))),
            dma((2, max(group, lines))),
        ],
        compiler_params=pltpu.CompilerParams(collective_id=0, has_side_effects=True),
        cost_estimate=pl.CostEstimate(flops=flops, bytes_accessed=5 * count * length * length * 2, transcendentals=0),
    )(
        patches.reshape(count, length, length),
        offsets,
        offsets,
        valid_masks.reshape(3, rows_dev, columns),
        initial_positions.reshape(2, nodes_rows, nodes_cols),
        *[jnp.asarray(table) for table in tables(length)],
    )
    positions, targets, surfaces, norms = outs
    return (
        positions.reshape(initial_positions.shape),
        targets.reshape(peak_offsets.shape),
        surfaces.reshape(1, 3, rows_dev, columns, length, length),
        norms[:, 0],
    )


def solution(mesh):
    depth, tiles = mesh.shape["gz"], mesh.shape["xy"]
    placed = (
        P("gz", "xy", None, None, None),
        P("gz", None, "xy", None),
        P("gz", None, "xy", None),
        P(None, "gz", "xy", None),
    )
    return jax.shard_map(
        functools.partial(local, depth, tiles),
        mesh=mesh,
        in_specs=placed,
        out_specs=(
            P(None, "gz", "xy", None),
            P("gz", None, "xy", None),
            P("gz", None, "xy", None, None, None),
            P(),
        ),
        check_vma=False,
    )
```

```python
import functools

import numpy as np

import jax
import jax.numpy as jnp
from jax import lax
from jax.experimental import pallas as pl
from jax.experimental.pallas import tpu as pltpu
from jax.sharding import PartitionSpec as P

SUB = 16
ITERS = 4
LINE = 4
CHUNKS = 16
AHEAD = 4
OWN_STEP = 8
LAG = 2

lattice_stiff = 0.5
clip_level = 5.0
step_size = 0.2
floor_ratio = 0.4
tiny_eps = 1e-06

MESH = pl.DeviceIdType.MESH
F32 = jnp.float32
BF16 = jnp.bfloat16
PAIRS = [(i, j) for i in range(ITERS) for j in range(i, ITERS)]


def tables(length):
    series = np.arange(length)
    angles = 2.0 * np.pi / length * (series[:, None] * series[None, :] % length)
    cosine = np.cos(angles).astype(jnp.bfloat16)
    sine = np.sin(angles).astype(jnp.bfloat16)
    right = np.concatenate([cosine, sine], axis=1)
    left = np.block([[cosine, -sine], [-sine, -cosine]])
    back = np.block([[cosine, sine], [-sine, cosine]])
    last = np.concatenate([cosine, -sine], axis=1)
    return np.concatenate([right, left, back, last], axis=0)


def kernel(
    depth,
    tiles,
    patches,
    offsets_h,
    masks_h,
    start_h,
    tables_h,
    targets,
    surfaces,
    fields,
    gram_out,
    own,
    near,
    passing,
    spec_real,
    spec_imag,
    staged,
    offsets,
    offsets_v,
    masks,
    start,
    table,
    taps,
    send_z,
    recv_z,
    send_e,
    recv_e,
    weight_t,
    weight_l,
    target_t,
    target_l,
    weights,
    gram,
    gram_row,
    gram_a,
    gram_b,
    local_sem,
    in_sem,
    surf_sem,
    ps,
    pr,
    zs,
    zr,
    es,
    er,
    ws,
    wr,
    ts,
    tr,
    gs,
    gr,
):
    z = lax.axis_index("gz")
    t = lax.axis_index("xy")
    count, length, _ = own.shape
    piece = count // CHUNKS
    columns = masks_h.shape[2]
    rows_dev = masks_h.shape[1]
    lines = depth // LINE
    y = lax.rem(z, LINE)
    line = lax.div(z, LINE)
    has_next = line < lines - 1
    has_prev = line > 0
    group = LINE * tiles
    me = y * tiles + t

    def remote(src, dst, send, recv, gz, xy):
        return pltpu.make_async_remote_copy(
            src_ref=src, dst_ref=dst, send_sem=send, recv_sem=recv, device_id=(gz, xy), device_id_type=MESH
        )

    def local_copy(c):
        part = pl.ds(c * piece, piece)
        return pltpu.make_async_copy(patches.at[part], own.at[part], local_sem.at[c])

    inputs = [
        pltpu.make_async_copy(source, held, in_sem.at[n])
        for n, (source, held) in enumerate(
            ((masks_h, masks), (start_h, start), (offsets_h, offsets_v), (offsets_h, offsets), (tables_h, table))
        )
    ]
    for copy in inputs:
        copy.start()
    right = table.at[0:length]
    left = table.at[length : 3 * length]
    back = table.at[3 * length : 5 * length]
    last = table.at[5 * length : 6 * length]

    def start_local(c, carry):
        local_copy(c).start()
        return carry

    lax.fori_loop(0, CHUNKS, start_local, 0)

    barrier = pltpu.get_barrier_semaphore()

    def greet_group(i, carry):
        other = lax.rem(me + i, group)
        gz = line * LINE + lax.div(other, tiles)
        pl.semaphore_signal(barrier, inc=1, device_id=(gz, lax.rem(other, tiles)), device_id_type=MESH)
        return carry

    lax.fori_loop(1, group, greet_group, 0)

    def greet_lines(i, carry):
        other = lax.rem(line + i, lines)
        pl.semaphore_signal(barrier, inc=1, device_id=(other * LINE + y, t), device_id_type=MESH)
        return carry

    lax.fori_loop(1, lines, greet_lines, 0)
    for k in range(1, 4):
        for sign in (-1, 1):
            there = z + sign * k

            @pl.when((there >= 0) & (there < depth))
            def _():
                pl.semaphore_signal(barrier, inc=1, device_id=(there, t), device_id_type=MESH)

    for k in range(1, 4):

        @pl.when(z + k >= depth)
        def _():
            near[k - 1] = jnp.zeros(near.shape[1:], BF16)
            for r in range(ITERS):
                recv_z[r, k - 1] = jnp.zeros(recv_z.shape[2:], BF16)

        @pl.when(z - k < 0)
        def _():
            for r in range(ITERS):
                recv_z[r, 2 + k] = jnp.zeros(recv_z.shape[2:], BF16)
            weight_l[k - 1] = jnp.zeros(weight_l.shape[1:], F32)
            target_l[k - 1] = jnp.zeros(target_l.shape[1:], F32)

    inputs[0].wait()
    inputs[1].wait()
    weight_t[...] = jnp.zeros(weight_t.shape, F32)
    target_t[...] = jnp.zeros(target_t.shape, F32)
    taps[...] = jnp.zeros(taps.shape, F32)
    for k in range(1, 4):
        live = jnp.where(z + k < depth, 1.0 / k, 0.0).astype(F32)
        weight_t[2 * (k - 1) : 2 * k, 0:columns] = masks[k - 1].astype(F32) * live

    def stage(r, value):
        for a in range(2):
            send_z[r, a] = value[a].astype(BF16)
            send_e[r, 0, a : a + 1] = value[a][0:1]
            send_e[r, 1, a : a + 1] = value[a][-1:]

    start_value = [start[0], start[1]]
    stage(0, start_value)

    for copy in inputs[2:]:
        copy.wait()
    half = length

    def dot(a, b):
        return jnp.dot(a, b, preferred_element_type=F32)

    def side_by_side(m):
        return jnp.concatenate(
            [
                jnp.concatenate([m[:half, :half], m[half:, :half]], axis=1),
                jnp.concatenate([m[:half, half:], m[half:, half:]], axis=1),
            ],
            axis=0,
        )

    def spectra(sources):
        mixed = [dot(ref[pl.ds(p, 2)].reshape(2 * half, half), right[...]).astype(BF16) for ref, p in sources]
        return [dot(left[...], side_by_side(m)) for m in mixed]

    def own_spectra(i, carry):
        firsts = [OWN_STEP * i + 2 * n for n in range(OWN_STEP // 2)]
        for p, s in zip(firsts, spectra([(own, p) for p in firsts])):
            for a in range(2):
                cols = slice(a * half, (a + 1) * half)
                spec_real[p + a] = s[:half, cols]
                spec_imag[p + a] = s[half:, cols]
        return carry

    def wait_local(c, carry):
        local_copy(c).wait()
        return carry

    lax.fori_loop(0, CHUNKS, wait_local, 0)
    lax.fori_loop(0, count // OWN_STEP, own_spectra, 0)

    expected = group - 1 + lines - 1
    for k in range(1, 4):
        expected = expected + (z + k < depth).astype(jnp.int32) + (z - k >= 0).astype(jnp.int32)
    pl.semaphore_wait(barrier, expected)

    def z_copy(r, k, sign):
        slot = 2 + k if sign > 0 else k - 1
        return remote(send_z.at[r], recv_z.at[r, slot], zs.at[r, slot], zr.at[r, slot], z + sign * k, t)

    def e_copy(r, sign):
        side = 1 if sign > 0 else 0
        return remote(send_e.at[r, side], recv_e.at[r, 1 - side], es.at[r, side], er.at[r, 1 - side], z, t + sign)

    def exchange_start(r):
        for k in (3, 2, 1):
            for sign in (-1, 1):

                @pl.when((z + sign * k >= 0) & (z + sign * k < depth))
                def _():
                    z_copy(r, k, sign).start()

        for sign in (-1, 1):

            @pl.when((t + sign >= 0) & (t + sign < tiles))
            def _():
                e_copy(r, sign).start()

    def exchange_wait(r):
        for k in (1, 2, 3):
            for sign in (-1, 1):

                @pl.when((z - sign * k >= 0) & (z - sign * k < depth))
                def _():
                    z_copy(r, k, sign).wait_recv()

        for sign in (-1, 1):

            @pl.when((t - sign >= 0) & (t - sign < tiles))
            def _():
                e_copy(r, sign).wait_recv()

    def exchange_drain(r):
        for k in (1, 2, 3):
            for sign in (-1, 1):

                @pl.when((z + sign * k >= 0) & (z + sign * k < depth))
                def _():
                    z_copy(r, k, sign).wait_send()

        for sign in (-1, 1):

            @pl.when((t + sign >= 0) & (t + sign < tiles))
            def _():
                e_copy(r, sign).wait_send()

    def w_copy(k):
        return remote(weight_t, weight_l.at[k - 1], ws.at[k - 1], wr.at[k - 1], z + k, t)

    def t_copy(k):
        return remote(target_t.at[k - 1], target_l.at[k - 1], ts.at[k - 1], tr.at[k - 1], z + k, t)

    def part_of(c):
        return pl.ds(c * piece, piece)

    def patch_copy(src, dst, send, slot, c, gz):
        part = part_of(c)
        return remote(src.at[part], dst.at[part], ps.at[send], pr.at[slot, c], gz, t)

    relays = (y == 1) | (y == 2)
    own_sends = [
        (z >= 3, own, near.at[2], 0, 2, z - 3),
        (y >= 1, own, near.at[0], 1, 0, z - 1),
        ((y == 0) & has_prev, own, passing, 2, 3, z + 3),
    ]
    pass_sends = [((y == LINE - 1) & has_prev, passing, near.at[0], 3, 0, z - LINE)]
    first_sends = [(relays, near.at[0], near.at[1], 4, 1, z - 1)]
    third_sends = [(relays & has_next, near.at[2], near.at[1], 5, 1, z + 1)]
    all_sends = own_sends + pass_sends + first_sends + third_sends

    def send_all(sends, c):
        for condition, src, dst, send, slot, gz in sends:

            @pl.when(condition)
            def _():
                patch_copy(src, dst, send, slot, c, gz).start()

    def arrived(slot, c):
        buffer = passing if slot == 3 else near.at[slot]
        patch_copy(buffer, buffer, 0, slot, c, z).wait_recv()

    exchange_start(0)
    for k in range(1, 4):

        @pl.when(z + k < depth)
        def _():
            w_copy(k).start()

    def send_own(c, carry):
        send_all(own_sends, c)
        return carry

    lax.fori_loop(0, AHEAD, send_own, 0)

    row_id = lax.broadcasted_iota(jnp.int32, (16, length), 0)
    row_id = jnp.where(row_id < 8, row_id, row_id - 16)
    col_id = lax.broadcasted_iota(jnp.int32, (16, length), 1)
    col_id = jnp.where(col_id < length // 2, col_id, col_id - length)
    tap_row = lax.broadcasted_iota(jnp.int32, (8, length), 0)
    tap_col = lax.broadcasted_iota(jnp.int32, (8, length), 1)

    def pick(k, p, window):
        r = lax.div(p, columns)
        c = lax.rem(p, columns)
        d_row = row_id - offsets[2 * k, r, c]
        d_col = col_id - offsets[2 * k + 1, r, c]
        down = jnp.where((d_col == 0) & (jnp.abs(d_row) <= 1), window, 0.0)
        across = jnp.where((d_row == 0) & (jnp.abs(d_col) <= 1), window, 0.0)

        def total(v):
            return jnp.sum(jnp.sum(v, axis=0, keepdims=True), axis=1, keepdims=True)

        sums = (
            total(down * d_row.astype(F32)),
            total(jnp.abs(down)),
            total(across * d_col.astype(F32)),
            total(jnp.abs(across)),
        )
        value = taps[k]
        for q in range(4):
            value = jnp.where((tap_row == 2 * q + r) & (tap_col == c), sums[q], value)
        taps[k] = value

    def correlate(works):
        pairs = [(k, c * piece + 2 * i) for i in range(piece // 2) for k, c in works]
        crossed = []
        for (k, p), s in zip(pairs, spectra([(near.at[k], p) for k, p in pairs])):
            mixed = []
            for a in range(2):
                cols = slice(a * half, (a + 1) * half)
                b_real, b_imag = s[:half, cols], s[half:, cols]
                a_real, a_imag = spec_real[p + a], spec_imag[p + a]
                real = (a_real * b_real + a_imag * b_imag).astype(BF16)
                imag = (a_real * b_imag - a_imag * b_real).astype(BF16)
                mixed.append(jnp.concatenate([real, imag], axis=1))
            crossed.append(jnp.concatenate(mixed, axis=0))
        halves = [dot(m, back[...]).astype(BF16) for m in crossed]
        corrs = [dot(last[...], side_by_side(h)) * (1.0 / (length * length)) for h in halves]
        for (k, p), corr in zip(pairs, corrs):
            for a in range(2):
                one = corr[:, a * half : (a + 1) * half]
                staged[k, p + a] = one.astype(BF16)
                pick(k, p + a, jnp.concatenate([one[:8], one[length - 8 :]], axis=0))
        for k, c in works:
            part = part_of(c)
            pltpu.make_async_copy(staged.at[k, part], surfaces.at[k, part], surf_sem).start()

    late = jnp.where(y == LINE - 1, LAG, 0)

    def step(c, carry):
        @pl.when(c < CHUNKS - AHEAD)
        def _():
            send_own(c + AHEAD, 0)

        c_0 = c - late
        c_1 = c - LAG
        has_0 = (c_0 >= 0) & (c_0 < CHUNKS)

        @pl.when(c < CHUNKS)
        def _():
            @pl.when((y == LINE - 1) & has_prev)
            def _():
                arrived(3, c)

            send_all(pass_sends, c)

            @pl.when(z + 3 < depth)
            def _():
                arrived(2, c)

            send_all(third_sends, c)

        @pl.when(has_0)
        def _():
            @pl.when(z + 1 < depth)
            def _():
                arrived(0, c_0)

            send_all(first_sends, c_0)

        @pl.when((c_1 >= 0) & (z + 2 < depth))
        def _():
            arrived(1, c_1)

        steady = (c_1 >= 0) & (c < CHUNKS)

        @pl.when(steady)
        def _():
            correlate([(2, c), (0, c_0), (1, c_1)])

        @pl.when(jnp.logical_not(steady) & (c < CHUNKS))
        def _():
            correlate([(2, c)])

        @pl.when(jnp.logical_not(steady) & has_0)
        def _():
            correlate([(0, c_0)])

        @pl.when(jnp.logical_not(steady) & (c_1 >= 0))
        def _():
            correlate([(1, c_1)])

        return carry

    lax.fori_loop(0, CHUNKS + LAG, step, 0)

    for k in range(1, 4):
        sums = taps[k - 1]
        weight = weight_t[2 * (k - 1) : 2 * k, 0:columns]
        for a in range(2):
            slope = sums[4 * a : 4 * a + 2, 0:columns]
            size = sums[4 * a + 2 : 4 * a + 4, 0:columns]
            shift = offsets_v[2 * (k - 1) + a].astype(F32)
            value = shift + slope / jnp.maximum(size, floor_ratio * length)
            targets[2 * (k - 1) + a] = value
            target_t[k - 1, 2 * a : 2 * a + 2, 0:columns] = weight * value
    for k in range(1, 4):

        @pl.when(z + k < depth)
        def _():
            t_copy(k).start()

    nodes_rows, nodes_cols = start.shape[1], start.shape[2]
    spread = (
        lax.broadcasted_iota(jnp.int32, (length, nodes_cols), 0)
        == lax.shift_right_logical(lax.broadcasted_iota(jnp.int32, (length, nodes_cols), 1), 4)
    ).astype(F32)

    def widen(small):
        return jnp.dot(small, spread, precision=lax.Precision.HIGHEST, preferred_element_type=F32)

    def tall(wide, first):
        return jnp.concatenate(
            [jnp.broadcast_to(wide[first + r : first + r + 1], (SUB, nodes_cols)) for r in range(rows_dev)], axis=0
        )

    wide_own = widen(weight_t[...])
    for k in range(1, 4):

        @pl.when(z - k >= 0)
        def _():
            w_copy(k).wait_recv()

        weights[k - 1] = tall(wide_own, 2 * (k - 1))
        weights[2 + k] = tall(widen(weight_l[k - 1]), 2 * (k - 1))

    node_row = lax.broadcasted_iota(jnp.int32, (nodes_rows, nodes_cols), 0)
    node_col = lax.broadcasted_iota(jnp.int32, (nodes_rows, nodes_cols), 1)

    def linear(r, value):
        result = []
        for a in range(2):
            u = value[a]
            upper = jnp.where(t == 0, u[0:1], recv_e[r, 0, a : a + 1])
            lower = jnp.where(t == tiles - 1, u[-1:], recv_e[r, 1, a : a + 1])
            up = jnp.where(node_row == 0, upper, pltpu.roll(u, 1, 0))
            down = jnp.where(node_row == nodes_rows - 1, lower, pltpu.roll(u, nodes_rows - 1, 0))
            west = jnp.where(node_col == 0, u, pltpu.roll(u, 1, 1))
            east = jnp.where(node_col == nodes_cols - 1, u, pltpu.roll(u, nodes_cols - 1, 1))
            force = lattice_stiff * (up + down + west + east - 4.0 * u)
            for k in range(1, 4):
                force = force + weights[k - 1] * (recv_z[r, k - 1, a].astype(F32) - u)
                force = force - weights[2 + k] * (u - recv_z[r, 2 + k, a].astype(F32))
            result.append(force)
        return result

    exchange_wait(0)
    base = linear(0, start_value)

    for k in range(1, 4):

        @pl.when(z - k >= 0)
        def _():
            t_copy(k).wait_recv()

    pull = target_l[0] + target_l[1] + target_l[2] - target_t[0] - target_t[1] - target_t[2]
    wide_pull = widen(pull)
    value = [base[a] + tall(wide_pull, 2 * a) for a in range(2)]
    for i in range(ITERS):
        for a in range(2):
            fields[i, a] = value[a]
        if i < ITERS - 1:
            stage(i + 1, value)
            exchange_start(i + 1)
        for n, (first, second) in enumerate(PAIRS):
            if second == i:
                product = fields[first, 0] * value[0] + fields[first, 1] * value[1]
                row = jnp.sum(product, axis=0, keepdims=True)
                gram[n : n + 1] = row[:, :length] + row[:, length:]
        if i < ITERS - 1:
            exchange_wait(i + 1)
            moved = linear(i + 1, value)
            value = [value[a] + step_size * moved[a] for a in range(2)]

    def group_copy(i):
        other = lax.rem(me + i, group)
        return remote(
            gram_row.at[0],
            gram_a.at[me],
            gs.at[0, i],
            gr.at[0, i],
            line * LINE + lax.div(other, tiles),
            lax.rem(other, tiles),
        )

    def lines_copy(i):
        other = lax.rem(line + i, lines)
        return remote(gram_row.at[1], gram_b.at[line], gs.at[1, i], gr.at[1, i], other * LINE + y, t)

    def run(copy, number, what):
        def body(i, carry):
            getattr(copy(i), what)()
            return carry

        lax.fori_loop(1, number, body, 0)

    for n in range(len(PAIRS), gram.shape[0]):
        gram[n : n + 1] = jnp.zeros((1, length), F32)
    summed = jnp.sum(gram[...], axis=1, keepdims=True)
    on_row = lax.broadcasted_iota(jnp.int32, gram.shape, 0) == lax.broadcasted_iota(jnp.int32, gram.shape, 1)
    mine = jnp.sum(jnp.where(on_row, summed, 0.0), axis=0, keepdims=True)
    gram_row[0] = mine
    run(group_copy, group, "start")
    gram_a[me] = mine
    run(group_copy, group, "wait")
    total = gram_a[0]
    for i in range(1, group):
        total = total + gram_a[i]
    gram_row[1] = total
    run(lines_copy, lines, "start")
    gram_b[line] = total
    run(lines_copy, lines, "wait")
    total = gram_b[0]
    for i in range(1, lines):
        total = total + gram_b[i]
    gram_out[...] = jnp.broadcast_to(jnp.sum(jnp.where(on_row, total, 0.0), axis=1, keepdims=True), gram.shape)

    for k in range(1, 4):

        @pl.when(z + k < depth)
        def _():
            w_copy(k).wait_send()
            t_copy(k).wait_send()

    for r in range(ITERS):
        exchange_drain(r)
    for condition, src, dst, send, slot, gz in all_sends:

        @pl.when(condition)
        def _():
            remote(src, dst, ps.at[send], pr.at[slot, 0], gz, t).wait_send()

    pltpu.make_async_copy(staged, surfaces, surf_sem).wait()


def finish(number, start_h, fields_h, gram_h, targets_h, staged, positions, targets, surfaces, norms, held, start, fields, gram, sem_in, sem_out, sem):
    ways = [
        pltpu.make_async_copy(source, to, sem.at[n])
        for n, (source, to) in enumerate(((gram_h, gram), (start_h, start), (fields_h, fields), (targets_h, targets)))
    ]
    for copy in ways:
        copy.start()
    pieces = held.shape[0] // 4
    inward, outward = [], []
    for n in range(4):
        part = pl.ds(n * pieces, pieces)
        inward.append(pltpu.make_async_copy(staged.at[part], held.at[part], sem_in.at[n]))
        outward.append(pltpu.make_async_copy(held.at[part], surfaces.at[part], sem_out.at[n]))
        inward[n].start()
    for copy in ways:
        copy.wait()
    for n in range(4):
        inward[n].wait()
        outward[n].start()
    length = gram.shape[1]
    total = gram[...]

    entries = {}
    for n, (first, second) in enumerate(PAIRS):
        entries[first, second] = entries[second, first] = total[n : n + 1]
    ones = jnp.ones((1, length), F32)
    coefficients = [ones]
    sums = [jnp.zeros((1, length), F32)] * ITERS
    for i in range(ITERS):
        square = jnp.zeros((1, length), F32)
        for first in range(len(coefficients)):
            for second in range(len(coefficients)):
                square = square + coefficients[first] * coefficients[second] * entries[first, second]
        rms = jnp.sqrt(jnp.maximum(square, 0.0) / number + tiny_eps)
        norms[i] = rms[0, 0]
        factor = jnp.minimum(1.0, clip_level / rms)
        for n in range(len(coefficients)):
            sums[n] = sums[n] + step_size * factor * coefficients[n]
        kept = [(1.0 - factor) * value for value in coefficients] + [0.0 * ones]
        shifted = [0.0 * ones] + [factor * value for value in coefficients]
        coefficients = [kept[n] + shifted[n] for n in range(len(shifted))]
    for a in range(2):
        result = start[a]
        for n in range(ITERS):
            result = result + jnp.concatenate([sums[n], sums[n]], axis=1) * fields[n, a]
        positions[a] = result
    for copy in outward:
        copy.wait()


def local(depth, tiles, patches, peak_offsets, valid_masks, initial_positions):
    _, rows_dev, columns, length, _ = patches.shape
    count = rows_dev * columns
    _, _, nodes_rows, nodes_cols = initial_positions.shape
    offsets = peak_offsets.reshape(6, rows_dev, columns)
    vmem = pl.BlockSpec(memory_space=pltpu.VMEM)
    smem = pl.BlockSpec(memory_space=pltpu.SMEM)
    hbm = pl.BlockSpec(memory_space=pltpu.HBM)
    group = LINE * tiles
    lines = depth // LINE
    dma = pltpu.SemaphoreType.DMA
    flops = 2 * count * (4 * 6 + 3 * 6) * length**3
    start = initial_positions.reshape(2, nodes_rows, nodes_cols)
    targets, staged, fields, gram = pl.pallas_call(
        functools.partial(kernel, depth, tiles),
        out_shape=(
            jax.ShapeDtypeStruct((6, rows_dev, columns), F32),
            jax.ShapeDtypeStruct((3, count, length, length), BF16),
            jax.ShapeDtypeStruct((ITERS, 2, nodes_rows, nodes_cols), F32),
            jax.ShapeDtypeStruct((16, length), F32),
        ),
        in_specs=[hbm, hbm, hbm, hbm, hbm],
        out_specs=(vmem, hbm, vmem, vmem),
        scratch_shapes=[
            pltpu.VMEM((count, length, length), BF16),
            pltpu.VMEM((3, count, length, length), BF16),
            pltpu.VMEM((count, length, length), BF16),
            pltpu.VMEM((count, length, length), F32),
            pltpu.VMEM((count, length, length), F32),
            pltpu.VMEM((3, count, length, length), BF16),
            pltpu.SMEM((6, rows_dev, columns), jnp.int32),
            pltpu.VMEM((6, rows_dev, columns), jnp.int32),
            pltpu.VMEM((3, rows_dev, columns), jnp.int32),
            pltpu.VMEM((2, nodes_rows, nodes_cols), F32),
            pltpu.VMEM((6 * length, 2 * length), BF16),
            pltpu.VMEM((3, 8, length), F32),
            pltpu.VMEM((ITERS, 2, nodes_rows, nodes_cols), BF16),
            pltpu.VMEM((ITERS, 6, 2, nodes_rows, nodes_cols), BF16),
            pltpu.VMEM((ITERS, 2, 8, nodes_cols), F32),
            pltpu.VMEM((ITERS, 2, 8, nodes_cols), F32),
            pltpu.VMEM((8, length), F32),
            pltpu.VMEM((3, 8, length), F32),
            pltpu.VMEM((3, 8, length), F32),
            pltpu.VMEM((3, 8, length), F32),
            pltpu.VMEM((6, nodes_rows, nodes_cols), F32),
            pltpu.VMEM((16, length), F32),
            pltpu.VMEM((2, 1, length), F32),
            pltpu.VMEM((group, 1, length), F32),
            pltpu.VMEM((lines, 1, length), F32),
            dma((CHUNKS,)),
            dma((5,)),
            dma,
            dma((6,)),
            dma((4, CHUNKS)),
            dma((ITERS, 6)),
            dma((ITERS, 6)),
            dma((ITERS, 2)),
            dma((ITERS, 2)),
            dma((3,)),
            dma((3,)),
            dma((3,)),
            dma((3,)),
            dma((2, max(group, lines))),
            dma((2, max(group, lines))),
        ],
        compiler_params=pltpu.CompilerParams(collective_id=0, has_side_effects=True),
        cost_estimate=pl.CostEstimate(flops=flops, bytes_accessed=5 * count * length * length * 2, transcendentals=0),
    )(
        patches.reshape(count, length, length),
        offsets,
        valid_masks.reshape(3, rows_dev, columns),
        start,
        jnp.asarray(tables(length)),
    )
    number = 2.0 * depth * tiles * nodes_rows * nodes_cols
    positions, targets, surfaces, norms = pl.pallas_call(
        functools.partial(finish, number),
        out_shape=(
            jax.ShapeDtypeStruct((2, nodes_rows, nodes_cols), F32),
            jax.ShapeDtypeStruct((6, rows_dev, columns), F32),
            jax.ShapeDtypeStruct((3 * count, length, length), BF16),
            jax.ShapeDtypeStruct((ITERS,), F32),
        ),
        in_specs=[hbm, hbm, hbm, hbm, hbm],
        out_specs=(vmem, vmem, hbm, smem),
        scratch_shapes=[
            pltpu.VMEM((3 * count, length, length), BF16),
            pltpu.VMEM((2, nodes_rows, nodes_cols), F32),
            pltpu.VMEM((ITERS, 2, nodes_rows, nodes_cols), F32),
            pltpu.VMEM((16, length), F32),
            dma((4,)),
            dma((4,)),
            dma((4,)),
        ],
    )(start, fields, gram, targets, staged.reshape(3 * count, length, length))
    return (
        positions.reshape(initial_positions.shape),
        targets.reshape(peak_offsets.shape),
        surfaces.reshape(1, 3, rows_dev, columns, length, length),
        norms,
    )


def solution(mesh):
    depth, tiles = mesh.shape["gz"], mesh.shape["xy"]
    placed = (
        P("gz", "xy", None, None, None),
        P("gz", None, "xy", None),
        P("gz", None, "xy", None),
        P(None, "gz", "xy", None),
    )
    return jax.shard_map(
        functools.partial(local, depth, tiles),
        mesh=mesh,
        in_specs=placed,
        out_specs=(
            P(None, "gz", "xy", None),
            P("gz", None, "xy", None),
            P("gz", None, "xy", None, None, None),
            P(),
        ),
        check_vma=False,
    )
```

```python
import functools

import numpy as np

import jax
import jax.numpy as jnp
from jax import lax
from jax.experimental import pallas as pl
from jax.experimental.pallas import tpu as pltpu
from jax.sharding import PartitionSpec as P

SUB = 16
ITERS = 4
LINE = 4
CHUNKS = 16
AHEAD = 4
OWN_STEP = 8
LAG = 2

lattice_stiff = 0.5
clip_level = 5.0
step_size = 0.2
floor_ratio = 0.4
tiny_eps = 1e-06

MESH = pl.DeviceIdType.MESH
F32 = jnp.float32
BF16 = jnp.bfloat16
PAIRS = [(i, j) for i in range(ITERS) for j in range(i, ITERS)]


def tables(length):
    series = np.arange(length)
    angles = 2.0 * np.pi / length * (series[:, None] * series[None, :] % length)
    cosine = np.cos(angles).astype(jnp.bfloat16)
    sine = np.sin(angles).astype(jnp.bfloat16)
    right = np.concatenate([cosine, sine], axis=1)
    left = np.block([[cosine, -sine], [-sine, -cosine]])
    back = np.block([[cosine, sine], [-sine, cosine]])
    last = np.concatenate([cosine, -sine], axis=1)
    return np.concatenate([right, left, back, last], axis=0)


def kernel(
    depth,
    tiles,
    patches,
    offsets_h,
    masks_h,
    start_h,
    tables_h,
    targets,
    surfaces,
    fields,
    gram_out,
    own,
    near,
    passing,
    spec_real,
    spec_imag,
    staged,
    offsets,
    offsets_v,
    masks,
    start,
    table,
    taps,
    send_z,
    recv_z,
    send_e,
    recv_e,
    weight_t,
    weight_l,
    target_t,
    target_l,
    weights,
    gram,
    gram_row,
    gram_a,
    gram_b,
    local_sem,
    in_sem,
    surf_sem,
    ps,
    pr,
    zs,
    zr,
    es,
    er,
    ws,
    wr,
    ts,
    tr,
    gs,
    gr,
):
    z = lax.axis_index("gz")
    t = lax.axis_index("xy")
    count, length, _ = own.shape
    piece = count // CHUNKS
    columns = masks_h.shape[2]
    rows_dev = masks_h.shape[1]
    lines = depth // LINE
    y = lax.rem(z, LINE)
    line = lax.div(z, LINE)
    has_next = line < lines - 1
    has_prev = line > 0
    group = LINE * tiles
    me = y * tiles + t

    def remote(src, dst, send, recv, gz, xy):
        return pltpu.make_async_remote_copy(
            src_ref=src, dst_ref=dst, send_sem=send, recv_sem=recv, device_id=(gz, xy), device_id_type=MESH
        )

    def local_copy(c):
        part = pl.ds(c * piece, piece)
        return pltpu.make_async_copy(patches.at[part], own.at[part], local_sem.at[c])

    inputs = [
        pltpu.make_async_copy(source, held, in_sem.at[n])
        for n, (source, held) in enumerate(
            ((masks_h, masks), (start_h, start), (offsets_h, offsets_v), (offsets_h, offsets), (tables_h, table))
        )
    ]
    for copy in inputs:
        copy.start()
    right = table.at[0:length]
    left = table.at[length : 3 * length]
    back = table.at[3 * length : 5 * length]
    last = table.at[5 * length : 6 * length]

    def start_local(c, carry):
        local_copy(c).start()
        return carry

    lax.fori_loop(0, CHUNKS, start_local, 0)

    barrier = pltpu.get_barrier_semaphore()

    def greet_group(i, carry):
        other = lax.rem(me + i, group)
        gz = line * LINE + lax.div(other, tiles)
        pl.semaphore_signal(barrier, inc=1, device_id=(gz, lax.rem(other, tiles)), device_id_type=MESH)
        return carry

    lax.fori_loop(1, group, greet_group, 0)

    def greet_lines(i, carry):
        other = lax.rem(line + i, lines)
        pl.semaphore_signal(barrier, inc=1, device_id=(other * LINE + y, t), device_id_type=MESH)
        return carry

    lax.fori_loop(1, lines, greet_lines, 0)
    for k in range(1, 4):
        for sign in (-1, 1):
            there = z + sign * k

            @pl.when((there >= 0) & (there < depth))
            def _():
                pl.semaphore_signal(barrier, inc=1, device_id=(there, t), device_id_type=MESH)

    for k in range(1, 4):

        @pl.when(z + k >= depth)
        def _():
            near[k - 1] = jnp.zeros(near.shape[1:], BF16)
            for r in range(ITERS):
                recv_z[r, k - 1] = jnp.zeros(recv_z.shape[2:], BF16)

        @pl.when(z - k < 0)
        def _():
            for r in range(ITERS):
                recv_z[r, 2 + k] = jnp.zeros(recv_z.shape[2:], BF16)
            weight_l[k - 1] = jnp.zeros(weight_l.shape[1:], F32)
            target_l[k - 1] = jnp.zeros(target_l.shape[1:], F32)

    inputs[0].wait()
    inputs[1].wait()
    weight_t[...] = jnp.zeros(weight_t.shape, F32)
    target_t[...] = jnp.zeros(target_t.shape, F32)
    taps[...] = jnp.zeros(taps.shape, F32)
    for k in range(1, 4):
        live = jnp.where(z + k < depth, 1.0 / k, 0.0).astype(F32)
        weight_t[2 * (k - 1) : 2 * k, 0:columns] = masks[k - 1].astype(F32) * live

    def stage(r, value):
        for a in range(2):
            send_z[r, a] = value[a].astype(BF16)
            send_e[r, 0, a : a + 1] = value[a][0:1]
            send_e[r, 1, a : a + 1] = value[a][-1:]

    start_value = [start[0], start[1]]
    stage(0, start_value)

    for copy in inputs[2:]:
        copy.wait()
    half = length

    def dot(a, b):
        return jnp.dot(a, b, preferred_element_type=F32)

    def side_by_side(m):
        return jnp.concatenate(
            [
                jnp.concatenate([m[:half, :half], m[half:, :half]], axis=1),
                jnp.concatenate([m[:half, half:], m[half:, half:]], axis=1),
            ],
            axis=0,
        )

    def spectra(sources):
        mixed = [dot(ref[pl.ds(p, 2)].reshape(2 * half, half), right[...]).astype(BF16) for ref, p in sources]
        return [dot(left[...], side_by_side(m)) for m in mixed]

    def own_spectra(i, carry):
        firsts = [OWN_STEP * i + 2 * n for n in range(OWN_STEP // 2)]
        for p, s in zip(firsts, spectra([(own, p) for p in firsts])):
            for a in range(2):
                cols = slice(a * half, (a + 1) * half)
                spec_real[p + a] = s[:half, cols]
                spec_imag[p + a] = s[half:, cols]
        return carry

    def wait_local(c, carry):
        local_copy(c).wait()
        return carry

    lax.fori_loop(0, CHUNKS, wait_local, 0)
    lax.fori_loop(0, count // OWN_STEP, own_spectra, 0)

    expected = group - 1 + lines - 1
    for k in range(1, 4):
        expected = expected + (z + k < depth).astype(jnp.int32) + (z - k >= 0).astype(jnp.int32)
    pl.semaphore_wait(barrier, expected)

    def z_copy(r, k, sign):
        slot = 2 + k if sign > 0 else k - 1
        return remote(send_z.at[r], recv_z.at[r, slot], zs.at[r, slot], zr.at[r, slot], z + sign * k, t)

    def e_copy(r, sign):
        side = 1 if sign > 0 else 0
        return remote(send_e.at[r, side], recv_e.at[r, 1 - side], es.at[r, side], er.at[r, 1 - side], z, t + sign)

    def exchange_start(r):
        for k in (3, 2, 1):
            for sign in (-1, 1):

                @pl.when((z + sign * k >= 0) & (z + sign * k < depth))
                def _():
                    z_copy(r, k, sign).start()

        for sign in (-1, 1):

            @pl.when((t + sign >= 0) & (t + sign < tiles))
            def _():
                e_copy(r, sign).start()

    def exchange_wait(r):
        for k in (1, 2, 3):
            for sign in (-1, 1):

                @pl.when((z - sign * k >= 0) & (z - sign * k < depth))
                def _():
                    z_copy(r, k, sign).wait_recv()

        for sign in (-1, 1):

            @pl.when((t - sign >= 0) & (t - sign < tiles))
            def _():
                e_copy(r, sign).wait_recv()

    def exchange_drain(r):
        for k in (1, 2, 3):
            for sign in (-1, 1):

                @pl.when((z + sign * k >= 0) & (z + sign * k < depth))
                def _():
                    z_copy(r, k, sign).wait_send()

        for sign in (-1, 1):

            @pl.when((t + sign >= 0) & (t + sign < tiles))
            def _():
                e_copy(r, sign).wait_send()

    def w_copy(k):
        return remote(weight_t, weight_l.at[k - 1], ws.at[k - 1], wr.at[k - 1], z + k, t)

    def t_copy(k):
        return remote(target_t.at[k - 1], target_l.at[k - 1], ts.at[k - 1], tr.at[k - 1], z + k, t)

    def part_of(c):
        return pl.ds(c * piece, piece)

    def patch_copy(src, dst, send, slot, c, gz):
        part = part_of(c)
        return remote(src.at[part], dst.at[part], ps.at[send], pr.at[slot, c], gz, t)

    relays = (y == 1) | (y == 2)
    own_sends = [
        (z >= 3, own, near.at[2], 0, 2, z - 3),
        (y >= 1, own, near.at[0], 1, 0, z - 1),
        ((y == 0) & has_prev, own, passing, 2, 3, z + 3),
    ]
    pass_sends = [((y == LINE - 1) & has_prev, passing, near.at[0], 3, 0, z - LINE)]
    first_sends = [(relays, near.at[0], near.at[1], 4, 1, z - 1)]
    third_sends = [(relays & has_next, near.at[2], near.at[1], 5, 1, z + 1)]
    all_sends = own_sends + pass_sends + first_sends + third_sends

    def send_all(sends, c):
        for condition, src, dst, send, slot, gz in sends:

            @pl.when(condition)
            def _():
                patch_copy(src, dst, send, slot, c, gz).start()

    def arrived(slot, c):
        buffer = passing if slot == 3 else near.at[slot]
        patch_copy(buffer, buffer, 0, slot, c, z).wait_recv()

    for k in range(1, 4):

        @pl.when(z + k < depth)
        def _():
            w_copy(k).start()

    def send_own(c, carry):
        send_all(own_sends, c)
        return carry

    lax.fori_loop(0, AHEAD, send_own, 0)

    row_id = lax.broadcasted_iota(jnp.int32, (16, length), 0)
    row_id = jnp.where(row_id < 8, row_id, row_id - 16)
    col_id = lax.broadcasted_iota(jnp.int32, (16, length), 1)
    col_id = jnp.where(col_id < length // 2, col_id, col_id - length)
    tap_row = lax.broadcasted_iota(jnp.int32, (8, length), 0)
    tap_col = lax.broadcasted_iota(jnp.int32, (8, length), 1)

    def pick(k, p, window):
        r = lax.div(p, columns)
        c = lax.rem(p, columns)
        d_row = row_id - offsets[2 * k, r, c]
        d_col = col_id - offsets[2 * k + 1, r, c]
        down = jnp.where((d_col == 0) & (jnp.abs(d_row) <= 1), window, 0.0)
        across = jnp.where((d_row == 0) & (jnp.abs(d_col) <= 1), window, 0.0)

        def total(v):
            return jnp.sum(jnp.sum(v, axis=0, keepdims=True), axis=1, keepdims=True)

        sums = (
            total(down * d_row.astype(F32)),
            total(jnp.abs(down)),
            total(across * d_col.astype(F32)),
            total(jnp.abs(across)),
        )
        value = taps[k]
        for q in range(4):
            value = jnp.where((tap_row == 2 * q + r) & (tap_col == c), sums[q], value)
        taps[k] = value

    def correlate(works):
        pairs = [(k, c * piece + 2 * i) for i in range(piece // 2) for k, c in works]
        crossed = []
        for (k, p), s in zip(pairs, spectra([(near.at[k], p) for k, p in pairs])):
            mixed = []
            for a in range(2):
                cols = slice(a * half, (a + 1) * half)
                b_real, b_imag = s[:half, cols], s[half:, cols]
                a_real, a_imag = spec_real[p + a], spec_imag[p + a]
                real = (a_real * b_real + a_imag * b_imag).astype(BF16)
                imag = (a_real * b_imag - a_imag * b_real).astype(BF16)
                mixed.append(jnp.concatenate([real, imag], axis=1))
            crossed.append(jnp.concatenate(mixed, axis=0))
        halves = [dot(m, back[...]).astype(BF16) for m in crossed]
        corrs = [dot(last[...], side_by_side(h)) * (1.0 / (length * length)) for h in halves]
        for (k, p), corr in zip(pairs, corrs):
            for a in range(2):
                one = corr[:, a * half : (a + 1) * half]
                staged[k, p + a] = one.astype(BF16)
                pick(k, p + a, jnp.concatenate([one[:8], one[length - 8 :]], axis=0))
        for k, c in works:
            part = part_of(c)
            pltpu.make_async_copy(staged.at[k, part], surfaces.at[k, part], surf_sem).start()

    late = jnp.where(y == LINE - 1, LAG, 0)

    def step(c, carry):
        @pl.when(c < CHUNKS - AHEAD)
        def _():
            send_own(c + AHEAD, 0)

        @pl.when(c == 14)
        def _():
            exchange_start(0)

        c_0 = c - late
        c_1 = c - LAG
        has_0 = (c_0 >= 0) & (c_0 < CHUNKS)

        @pl.when(c < CHUNKS)
        def _():
            @pl.when((y == LINE - 1) & has_prev)
            def _():
                arrived(3, c)

            send_all(pass_sends, c)

            @pl.when(z + 3 < depth)
            def _():
                arrived(2, c)

            send_all(third_sends, c)

        @pl.when(has_0)
        def _():
            @pl.when(z + 1 < depth)
            def _():
                arrived(0, c_0)

            send_all(first_sends, c_0)

        @pl.when((c_1 >= 0) & (z + 2 < depth))
        def _():
            arrived(1, c_1)

        steady = (c_1 >= 0) & (c < CHUNKS)

        @pl.when(steady)
        def _():
            correlate([(2, c), (0, c_0), (1, c_1)])

        @pl.when(jnp.logical_not(steady) & (c < CHUNKS))
        def _():
            correlate([(2, c)])

        @pl.when(jnp.logical_not(steady) & has_0)
        def _():
            correlate([(0, c_0)])

        @pl.when(jnp.logical_not(steady) & (c_1 >= 0))
        def _():
            correlate([(1, c_1)])

        return carry

    lax.fori_loop(0, CHUNKS + LAG, step, 0)

    for k in range(1, 4):
        sums = taps[k - 1]
        weight = weight_t[2 * (k - 1) : 2 * k, 0:columns]
        for a in range(2):
            slope = sums[4 * a : 4 * a + 2, 0:columns]
            size = sums[4 * a + 2 : 4 * a + 4, 0:columns]
            shift = offsets_v[2 * (k - 1) + a].astype(F32)
            value = shift + slope / jnp.maximum(size, floor_ratio * length)
            targets[2 * (k - 1) + a] = value
            target_t[k - 1, 2 * a : 2 * a + 2, 0:columns] = weight * value
    for k in range(1, 4):

        @pl.when(z + k < depth)
        def _():
            t_copy(k).start()

    nodes_rows, nodes_cols = start.shape[1], start.shape[2]
    spread = (
        lax.broadcasted_iota(jnp.int32, (length, nodes_cols), 0)
        == lax.shift_right_logical(lax.broadcasted_iota(jnp.int32, (length, nodes_cols), 1), 4)
    ).astype(F32)

    def widen(small):
        return jnp.dot(small, spread, precision=lax.Precision.HIGHEST, preferred_element_type=F32)

    def tall(wide, first):
        return jnp.concatenate(
            [jnp.broadcast_to(wide[first + r : first + r + 1], (SUB, nodes_cols)) for r in range(rows_dev)], axis=0
        )

    wide_own = widen(weight_t[...])
    for k in range(1, 4):

        @pl.when(z - k >= 0)
        def _():
            w_copy(k).wait_recv()

        weights[k - 1] = tall(wide_own, 2 * (k - 1))
        weights[2 + k] = tall(widen(weight_l[k - 1]), 2 * (k - 1))

    node_row = lax.broadcasted_iota(jnp.int32, (nodes_rows, nodes_cols), 0)
    node_col = lax.broadcasted_iota(jnp.int32, (nodes_rows, nodes_cols), 1)

    def linear(r, value):
        result = []
        for a in range(2):
            u = value[a]
            upper = jnp.where(t == 0, u[0:1], recv_e[r, 0, a : a + 1])
            lower = jnp.where(t == tiles - 1, u[-1:], recv_e[r, 1, a : a + 1])
            up = jnp.where(node_row == 0, upper, pltpu.roll(u, 1, 0))
            down = jnp.where(node_row == nodes_rows - 1, lower, pltpu.roll(u, nodes_rows - 1, 0))
            west = jnp.where(node_col == 0, u, pltpu.roll(u, 1, 1))
            east = jnp.where(node_col == nodes_cols - 1, u, pltpu.roll(u, nodes_cols - 1, 1))
            force = lattice_stiff * (up + down + west + east - 4.0 * u)
            for k in range(1, 4):
                force = force + weights[k - 1] * (recv_z[r, k - 1, a].astype(F32) - u)
                force = force - weights[2 + k] * (u - recv_z[r, 2 + k, a].astype(F32))
            result.append(force)
        return result

    exchange_wait(0)
    base = linear(0, start_value)

    for k in range(1, 4):

        @pl.when(z - k >= 0)
        def _():
            t_copy(k).wait_recv()

    pull = target_l[0] + target_l[1] + target_l[2] - target_t[0] - target_t[1] - target_t[2]
    wide_pull = widen(pull)
    value = [base[a] + tall(wide_pull, 2 * a) for a in range(2)]
    for i in range(ITERS):
        for a in range(2):
            fields[i, a] = value[a]
        if i < ITERS - 1:
            stage(i + 1, value)
            exchange_start(i + 1)
        for n, (first, second) in enumerate(PAIRS):
            if second == i:
                product = fields[first, 0] * value[0] + fields[first, 1] * value[1]
                row = jnp.sum(product, axis=0, keepdims=True)
                gram[n : n + 1] = row[:, :length] + row[:, length:]
        if i < ITERS - 1:
            exchange_wait(i + 1)
            moved = linear(i + 1, value)
            value = [value[a] + step_size * moved[a] for a in range(2)]

    def group_copy(i):
        other = lax.rem(me + i, group)
        return remote(
            gram_row.at[0],
            gram_a.at[me],
            gs.at[0, i],
            gr.at[0, i],
            line * LINE + lax.div(other, tiles),
            lax.rem(other, tiles),
        )

    def lines_copy(i):
        other = lax.rem(line + i, lines)
        return remote(gram_row.at[1], gram_b.at[line], gs.at[1, i], gr.at[1, i], other * LINE + y, t)

    def run(copy, number, what):
        def body(i, carry):
            getattr(copy(i), what)()
            return carry

        lax.fori_loop(1, number, body, 0)

    for n in range(len(PAIRS), gram.shape[0]):
        gram[n : n + 1] = jnp.zeros((1, length), F32)
    summed = jnp.sum(gram[...], axis=1, keepdims=True)
    on_row = lax.broadcasted_iota(jnp.int32, gram.shape, 0) == lax.broadcasted_iota(jnp.int32, gram.shape, 1)
    mine = jnp.sum(jnp.where(on_row, summed, 0.0), axis=0, keepdims=True)
    gram_row[0] = mine
    run(group_copy, group, "start")
    gram_a[me] = mine
    run(group_copy, group, "wait")
    total = gram_a[0]
    for i in range(1, group):
        total = total + gram_a[i]
    gram_row[1] = total
    run(lines_copy, lines, "start")
    gram_b[line] = total
    run(lines_copy, lines, "wait")
    total = gram_b[0]
    for i in range(1, lines):
        total = total + gram_b[i]
    gram_out[...] = jnp.broadcast_to(jnp.sum(jnp.where(on_row, total, 0.0), axis=1, keepdims=True), gram.shape)

    for k in range(1, 4):

        @pl.when(z + k < depth)
        def _():
            w_copy(k).wait_send()
            t_copy(k).wait_send()

    for r in range(ITERS):
        exchange_drain(r)
    for condition, src, dst, send, slot, gz in all_sends:

        @pl.when(condition)
        def _():
            remote(src, dst, ps.at[send], pr.at[slot, 0], gz, t).wait_send()

    pltpu.make_async_copy(staged, surfaces, surf_sem).wait()


def finish(number, start_h, fields_h, gram_h, targets_h, staged, positions, targets, surfaces, norms, held, start, fields, gram, sem_in, sem_out, sem):
    ways = [
        pltpu.make_async_copy(source, to, sem.at[n])
        for n, (source, to) in enumerate(((gram_h, gram), (start_h, start), (fields_h, fields), (targets_h, targets)))
    ]
    for copy in ways:
        copy.start()
    pieces = held.shape[0] // 4
    inward, outward = [], []
    for n in range(4):
        part = pl.ds(n * pieces, pieces)
        inward.append(pltpu.make_async_copy(staged.at[part], held.at[part], sem_in.at[n]))
        outward.append(pltpu.make_async_copy(held.at[part], surfaces.at[part], sem_out.at[n]))
        inward[n].start()
    for copy in ways:
        copy.wait()
    for n in range(4):
        inward[n].wait()
        outward[n].start()
    length = gram.shape[1]
    total = gram[...]

    entries = {}
    for n, (first, second) in enumerate(PAIRS):
        entries[first, second] = entries[second, first] = total[n : n + 1]
    ones = jnp.ones((1, length), F32)
    coefficients = [ones]
    sums = [jnp.zeros((1, length), F32)] * ITERS
    for i in range(ITERS):
        square = jnp.zeros((1, length), F32)
        for first in range(len(coefficients)):
            for second in range(len(coefficients)):
                square = square + coefficients[first] * coefficients[second] * entries[first, second]
        rms = jnp.sqrt(jnp.maximum(square, 0.0) / number + tiny_eps)
        norms[i] = rms[0, 0]
        factor = jnp.minimum(1.0, clip_level / rms)
        for n in range(len(coefficients)):
            sums[n] = sums[n] + step_size * factor * coefficients[n]
        kept = [(1.0 - factor) * value for value in coefficients] + [0.0 * ones]
        shifted = [0.0 * ones] + [factor * value for value in coefficients]
        coefficients = [kept[n] + shifted[n] for n in range(len(shifted))]
    for a in range(2):
        result = start[a]
        for n in range(ITERS):
            result = result + jnp.concatenate([sums[n], sums[n]], axis=1) * fields[n, a]
        positions[a] = result
    for copy in outward:
        copy.wait()


def local(depth, tiles, patches, peak_offsets, valid_masks, initial_positions):
    _, rows_dev, columns, length, _ = patches.shape
    count = rows_dev * columns
    _, _, nodes_rows, nodes_cols = initial_positions.shape
    offsets = peak_offsets.reshape(6, rows_dev, columns)
    vmem = pl.BlockSpec(memory_space=pltpu.VMEM)
    smem = pl.BlockSpec(memory_space=pltpu.SMEM)
    hbm = pl.BlockSpec(memory_space=pltpu.HBM)
    group = LINE * tiles
    lines = depth // LINE
    dma = pltpu.SemaphoreType.DMA
    flops = 2 * count * (4 * 6 + 3 * 6) * length**3
    start = initial_positions.reshape(2, nodes_rows, nodes_cols)
    targets, staged, fields, gram = pl.pallas_call(
        functools.partial(kernel, depth, tiles),
        out_shape=(
            jax.ShapeDtypeStruct((6, rows_dev, columns), F32),
            jax.ShapeDtypeStruct((3, count, length, length), BF16),
            jax.ShapeDtypeStruct((ITERS, 2, nodes_rows, nodes_cols), F32),
            jax.ShapeDtypeStruct((16, length), F32),
        ),
        in_specs=[hbm, hbm, hbm, hbm, hbm],
        out_specs=(vmem, hbm, vmem, vmem),
        scratch_shapes=[
            pltpu.VMEM((count, length, length), BF16),
            pltpu.VMEM((3, count, length, length), BF16),
            pltpu.VMEM((count, length, length), BF16),
            pltpu.VMEM((count, length, length), F32),
            pltpu.VMEM((count, length, length), F32),
            pltpu.VMEM((3, count, length, length), BF16),
            pltpu.SMEM((6, rows_dev, columns), jnp.int32),
            pltpu.VMEM((6, rows_dev, columns), jnp.int32),
            pltpu.VMEM((3, rows_dev, columns), jnp.int32),
            pltpu.VMEM((2, nodes_rows, nodes_cols), F32),
            pltpu.VMEM((6 * length, 2 * length), BF16),
            pltpu.VMEM((3, 8, length), F32),
            pltpu.VMEM((ITERS, 2, nodes_rows, nodes_cols), BF16),
            pltpu.VMEM((ITERS, 6, 2, nodes_rows, nodes_cols), BF16),
            pltpu.VMEM((ITERS, 2, 8, nodes_cols), F32),
            pltpu.VMEM((ITERS, 2, 8, nodes_cols), F32),
            pltpu.VMEM((8, length), F32),
            pltpu.VMEM((3, 8, length), F32),
            pltpu.VMEM((3, 8, length), F32),
            pltpu.VMEM((3, 8, length), F32),
            pltpu.VMEM((6, nodes_rows, nodes_cols), F32),
            pltpu.VMEM((16, length), F32),
            pltpu.VMEM((2, 1, length), F32),
            pltpu.VMEM((group, 1, length), F32),
            pltpu.VMEM((lines, 1, length), F32),
            dma((CHUNKS,)),
            dma((5,)),
            dma,
            dma((6,)),
            dma((4, CHUNKS)),
            dma((ITERS, 6)),
            dma((ITERS, 6)),
            dma((ITERS, 2)),
            dma((ITERS, 2)),
            dma((3,)),
            dma((3,)),
            dma((3,)),
            dma((3,)),
            dma((2, max(group, lines))),
            dma((2, max(group, lines))),
        ],
        compiler_params=pltpu.CompilerParams(collective_id=0, has_side_effects=True),
        cost_estimate=pl.CostEstimate(flops=flops, bytes_accessed=5 * count * length * length * 2, transcendentals=0),
    )(
        patches.reshape(count, length, length),
        offsets,
        valid_masks.reshape(3, rows_dev, columns),
        start,
        jnp.asarray(tables(length)),
    )
    number = 2.0 * depth * tiles * nodes_rows * nodes_cols
    positions, targets, surfaces, norms = pl.pallas_call(
        functools.partial(finish, number),
        out_shape=(
            jax.ShapeDtypeStruct((2, nodes_rows, nodes_cols), F32),
            jax.ShapeDtypeStruct((6, rows_dev, columns), F32),
            jax.ShapeDtypeStruct((3 * count, length, length), BF16),
            jax.ShapeDtypeStruct((ITERS,), F32),
        ),
        in_specs=[hbm, hbm, hbm, hbm, hbm],
        out_specs=(vmem, vmem, hbm, smem),
        scratch_shapes=[
            pltpu.VMEM((3 * count, length, length), BF16),
            pltpu.VMEM((2, nodes_rows, nodes_cols), F32),
            pltpu.VMEM((ITERS, 2, nodes_rows, nodes_cols), F32),
            pltpu.VMEM((16, length), F32),
            dma((4,)),
            dma((4,)),
            dma((4,)),
        ],
    )(start, fields, gram, targets, staged.reshape(3 * count, length, length))
    return (
        positions.reshape(initial_positions.shape),
        targets.reshape(peak_offsets.shape),
        surfaces.reshape(1, 3, rows_dev, columns, length, length),
        norms,
    )


def solution(mesh):
    depth, tiles = mesh.shape["gz"], mesh.shape["xy"]
    placed = (
        P("gz", "xy", None, None, None),
        P("gz", None, "xy", None),
        P("gz", None, "xy", None),
        P(None, "gz", "xy", None),
    )
    return jax.shard_map(
        functools.partial(local, depth, tiles),
        mesh=mesh,
        in_specs=placed,
        out_specs=(
            P(None, "gz", "xy", None),
            P("gz", None, "xy", None),
            P("gz", None, "xy", None, None, None),
            P(),
        ),
        check_vma=False,
    )
```

```python
import functools

import numpy as np

import jax
import jax.numpy as jnp
from jax import lax
from jax.experimental import pallas as pl
from jax.experimental.pallas import tpu as pltpu
from jax.sharding import PartitionSpec as P

SUB = 16
ITERS = 4
LINE = 4
CHUNKS = 16
AHEAD = 6
FAR_AHEAD = 3
OWN_STEP = 8
LAG = 2

lattice_stiff = 0.5
clip_level = 5.0
step_size = 0.2
floor_ratio = 0.4
tiny_eps = 1e-06

MESH = pl.DeviceIdType.MESH
F32 = jnp.float32
BF16 = jnp.bfloat16
PAIRS = [(i, j) for i in range(ITERS) for j in range(i, ITERS)]


def tables(length):
    series = np.arange(length)
    angles = 2.0 * np.pi / length * (series[:, None] * series[None, :] % length)
    cosine = np.cos(angles).astype(jnp.bfloat16)
    sine = np.sin(angles).astype(jnp.bfloat16)
    right = np.concatenate([cosine, sine], axis=1)
    left = np.block([[cosine, -sine], [-sine, -cosine]])
    back = np.block([[cosine, sine], [-sine, cosine]])
    last = np.concatenate([cosine, -sine], axis=1)
    return np.concatenate([right, left, back, last], axis=0)


def kernel(
    depth,
    tiles,
    patches,
    offsets_h,
    masks_h,
    start_h,
    tables_h,
    targets,
    surfaces,
    fields,
    gram_out,
    own,
    near,
    passing,
    spec_real,
    spec_imag,
    staged,
    offsets,
    offsets_v,
    masks,
    start,
    table,
    taps,
    send_z,
    recv_z,
    send_e,
    recv_e,
    weight_t,
    weight_l,
    target_t,
    target_l,
    weights,
    gram,
    gram_row,
    gram_a,
    gram_b,
    local_sem,
    in_sem,
    surf_sem,
    ps,
    pr,
    zs,
    zr,
    es,
    er,
    ws,
    wr,
    ts,
    tr,
    gs,
    gr,
):
    z = lax.axis_index("gz")
    t = lax.axis_index("xy")
    count, length, _ = own.shape
    piece = count // CHUNKS
    columns = masks_h.shape[2]
    rows_dev = masks_h.shape[1]
    lines = depth // LINE
    y = lax.rem(z, LINE)
    line = lax.div(z, LINE)
    has_next = line < lines - 1
    has_prev = line > 0
    group = LINE * tiles
    me = y * tiles + t

    def remote(src, dst, send, recv, gz, xy):
        return pltpu.make_async_remote_copy(
            src_ref=src, dst_ref=dst, send_sem=send, recv_sem=recv, device_id=(gz, xy), device_id_type=MESH
        )

    def local_copy(c):
        part = pl.ds(c * piece, piece)
        return pltpu.make_async_copy(patches.at[part], own.at[part], local_sem.at[c])

    inputs = [
        pltpu.make_async_copy(source, held, in_sem.at[n])
        for n, (source, held) in enumerate(
            ((masks_h, masks), (start_h, start), (offsets_h, offsets_v), (offsets_h, offsets), (tables_h, table))
        )
    ]
    for copy in inputs:
        copy.start()
    right = table.at[0:length]
    left = table.at[length : 3 * length]
    back = table.at[3 * length : 5 * length]
    last = table.at[5 * length : 6 * length]

    def start_local(c, carry):
        local_copy(c).start()
        return carry

    lax.fori_loop(0, CHUNKS, start_local, 0)

    barrier = pltpu.get_barrier_semaphore()

    def greet_group(i, carry):
        other = lax.rem(me + i, group)
        gz = line * LINE + lax.div(other, tiles)
        pl.semaphore_signal(barrier, inc=1, device_id=(gz, lax.rem(other, tiles)), device_id_type=MESH)
        return carry

    lax.fori_loop(1, group, greet_group, 0)

    def greet_lines(i, carry):
        other = lax.rem(line + i, lines)
        pl.semaphore_signal(barrier, inc=1, device_id=(other * LINE + y, t), device_id_type=MESH)
        return carry

    lax.fori_loop(1, lines, greet_lines, 0)
    for k in range(1, 4):
        for sign in (-1, 1):
            there = z + sign * k

            @pl.when((there >= 0) & (there < depth))
            def _():
                pl.semaphore_signal(barrier, inc=1, device_id=(there, t), device_id_type=MESH)

    for k in range(1, 4):

        @pl.when(z + k >= depth)
        def _():
            near[k - 1] = jnp.zeros(near.shape[1:], BF16)
            for r in range(ITERS):
                recv_z[r, k - 1] = jnp.zeros(recv_z.shape[2:], BF16)

        @pl.when(z - k < 0)
        def _():
            for r in range(ITERS):
                recv_z[r, 2 + k] = jnp.zeros(recv_z.shape[2:], BF16)
            weight_l[k - 1] = jnp.zeros(weight_l.shape[1:], F32)
            target_l[k - 1] = jnp.zeros(target_l.shape[1:], F32)

    inputs[0].wait()
    inputs[1].wait()
    weight_t[...] = jnp.zeros(weight_t.shape, F32)
    target_t[...] = jnp.zeros(target_t.shape, F32)
    taps[...] = jnp.zeros(taps.shape, F32)
    for k in range(1, 4):
        live = jnp.where(z + k < depth, 1.0 / k, 0.0).astype(F32)
        weight_t[2 * (k - 1) : 2 * k, 0:columns] = masks[k - 1].astype(F32) * live

    def stage(r, value):
        for a in range(2):
            send_z[r, a] = value[a].astype(BF16)
            send_e[r, 0, a : a + 1] = value[a][0:1]
            send_e[r, 1, a : a + 1] = value[a][-1:]

    start_value = [start[0], start[1]]
    stage(0, start_value)

    for copy in inputs[2:]:
        copy.wait()
    half = length

    def dot(a, b):
        return jnp.dot(a, b, preferred_element_type=F32)

    def side_by_side(m):
        return jnp.concatenate(
            [
                jnp.concatenate([m[:half, :half], m[half:, :half]], axis=1),
                jnp.concatenate([m[:half, half:], m[half:, half:]], axis=1),
            ],
            axis=0,
        )

    def spectra(sources):
        mixed = [dot(ref[pl.ds(p, 2)].reshape(2 * half, half), right[...]).astype(BF16) for ref, p in sources]
        return [dot(left[...], side_by_side(m)) for m in mixed]

    def own_spectra(i, carry):
        firsts = [OWN_STEP * i + 2 * n for n in range(OWN_STEP // 2)]
        for p, s in zip(firsts, spectra([(own, p) for p in firsts])):
            for a in range(2):
                cols = slice(a * half, (a + 1) * half)
                spec_real[p + a] = s[:half, cols]
                spec_imag[p + a] = s[half:, cols]
        return carry

    def wait_local(c, carry):
        local_copy(c).wait()
        return carry

    lax.fori_loop(0, CHUNKS, wait_local, 0)
    lax.fori_loop(0, count // OWN_STEP, own_spectra, 0)

    expected = group - 1 + lines - 1
    for k in range(1, 4):
        expected = expected + (z + k < depth).astype(jnp.int32) + (z - k >= 0).astype(jnp.int32)
    pl.semaphore_wait(barrier, expected)

    def z_copy(r, k, sign):
        slot = 2 + k if sign > 0 else k - 1
        return remote(send_z.at[r], recv_z.at[r, slot], zs.at[r, slot], zr.at[r, slot], z + sign * k, t)

    def e_copy(r, sign):
        side = 1 if sign > 0 else 0
        return remote(send_e.at[r, side], recv_e.at[r, 1 - side], es.at[r, side], er.at[r, 1 - side], z, t + sign)

    def exchange_start(r):
        for k in (3, 2, 1):
            for sign in (-1, 1):

                @pl.when((z + sign * k >= 0) & (z + sign * k < depth))
                def _():
                    z_copy(r, k, sign).start()

        for sign in (-1, 1):

            @pl.when((t + sign >= 0) & (t + sign < tiles))
            def _():
                e_copy(r, sign).start()

    def exchange_wait(r):
        for k in (1, 2, 3):
            for sign in (-1, 1):

                @pl.when((z - sign * k >= 0) & (z - sign * k < depth))
                def _():
                    z_copy(r, k, sign).wait_recv()

        for sign in (-1, 1):

            @pl.when((t - sign >= 0) & (t - sign < tiles))
            def _():
                e_copy(r, sign).wait_recv()

    def exchange_drain(r):
        for k in (1, 2, 3):
            for sign in (-1, 1):

                @pl.when((z + sign * k >= 0) & (z + sign * k < depth))
                def _():
                    z_copy(r, k, sign).wait_send()

        for sign in (-1, 1):

            @pl.when((t + sign >= 0) & (t + sign < tiles))
            def _():
                e_copy(r, sign).wait_send()

    def w_copy(k):
        return remote(weight_t, weight_l.at[k - 1], ws.at[k - 1], wr.at[k - 1], z + k, t)

    def t_copy(k):
        return remote(target_t.at[k - 1], target_l.at[k - 1], ts.at[k - 1], tr.at[k - 1], z + k, t)

    def part_of(c):
        return pl.ds(c * piece, piece)

    def patch_copy(src, dst, send, slot, c, gz):
        part = part_of(c)
        return remote(src.at[part], dst.at[part], ps.at[send], pr.at[slot, c], gz, t)

    relays = (y == 1) | (y == 2)
    far_sends = [
        (z >= 3, own, near.at[2], 0, 2, z - 3),
        ((y == 0) & has_prev, own, passing, 2, 3, z + 3),
    ]
    next_sends = [(y >= 1, own, near.at[0], 1, 0, z - 1)]
    pass_sends = [((y == LINE - 1) & has_prev, passing, near.at[0], 3, 0, z - LINE)]
    first_sends = [(relays, near.at[0], near.at[1], 4, 1, z - 1)]
    third_sends = [(relays & has_next, near.at[2], near.at[1], 5, 1, z + 1)]
    all_sends = far_sends + next_sends + pass_sends + first_sends + third_sends

    def send_all(sends, c):
        for condition, src, dst, send, slot, gz in sends:

            @pl.when(condition)
            def _():
                patch_copy(src, dst, send, slot, c, gz).start()

    def arrived(slot, c):
        buffer = passing if slot == 3 else near.at[slot]
        patch_copy(buffer, buffer, 0, slot, c, z).wait_recv()

    for k in range(1, 4):

        @pl.when(z + k < depth)
        def _():
            w_copy(k).start()

    def send_far(c, carry):
        send_all(far_sends, c)
        return carry

    def send_next(c, carry):
        send_all(next_sends, c)
        return carry

    lax.fori_loop(0, AHEAD, send_next, 0)
    lax.fori_loop(0, FAR_AHEAD, send_far, 0)

    row_id = lax.broadcasted_iota(jnp.int32, (16, length), 0)
    row_id = jnp.where(row_id < 8, row_id, row_id - 16)
    col_id = lax.broadcasted_iota(jnp.int32, (16, length), 1)
    col_id = jnp.where(col_id < length // 2, col_id, col_id - length)
    tap_row = lax.broadcasted_iota(jnp.int32, (8, length), 0)
    tap_col = lax.broadcasted_iota(jnp.int32, (8, length), 1)

    def pick(k, p, window):
        r = lax.div(p, columns)
        c = lax.rem(p, columns)
        d_row = row_id - offsets[2 * k, r, c]
        d_col = col_id - offsets[2 * k + 1, r, c]
        down = jnp.where((d_col == 0) & (jnp.abs(d_row) <= 1), window, 0.0)
        across = jnp.where((d_row == 0) & (jnp.abs(d_col) <= 1), window, 0.0)

        def total(v):
            return jnp.sum(jnp.sum(v, axis=0, keepdims=True), axis=1, keepdims=True)

        sums = (
            total(down * d_row.astype(F32)),
            total(jnp.abs(down)),
            total(across * d_col.astype(F32)),
            total(jnp.abs(across)),
        )
        value = taps[k]
        for q in range(4):
            value = jnp.where((tap_row == 2 * q + r) & (tap_col == c), sums[q], value)
        taps[k] = value

    def correlate(works):
        pairs = [(k, c * piece + 2 * i) for i in range(piece // 2) for k, c in works]
        crossed = []
        for (k, p), s in zip(pairs, spectra([(near.at[k], p) for k, p in pairs])):
            mixed = []
            for a in range(2):
                cols = slice(a * half, (a + 1) * half)
                b_real, b_imag = s[:half, cols], s[half:, cols]
                a_real, a_imag = spec_real[p + a], spec_imag[p + a]
                real = (a_real * b_real + a_imag * b_imag).astype(BF16)
                imag = (a_real * b_imag - a_imag * b_real).astype(BF16)
                mixed.append(jnp.concatenate([real, imag], axis=1))
            crossed.append(jnp.concatenate(mixed, axis=0))
        halves = [dot(m, back[...]).astype(BF16) for m in crossed]
        corrs = [dot(last[...], side_by_side(h)) * (1.0 / (length * length)) for h in halves]
        for (k, p), corr in zip(pairs, corrs):
            for a in range(2):
                one = corr[:, a * half : (a + 1) * half]
                staged[k, p + a] = one.astype(BF16)
                pick(k, p + a, jnp.concatenate([one[:8], one[length - 8 :]], axis=0))
        for k, c in works:
            part = part_of(c)
            pltpu.make_async_copy(staged.at[k, part], surfaces.at[k, part], surf_sem).start()

    late = jnp.where(y == LINE - 1, LAG, 0)

    def step(c, carry):
        @pl.when(c < CHUNKS - FAR_AHEAD)
        def _():
            send_far(c + FAR_AHEAD, 0)

        @pl.when(c < CHUNKS - AHEAD)
        def _():
            send_next(c + AHEAD, 0)

        @pl.when(c == CHUNKS)
        def _():
            exchange_start(0)

        c_0 = c - late
        c_1 = c - LAG
        has_0 = (c_0 >= 0) & (c_0 < CHUNKS)

        @pl.when(c < CHUNKS)
        def _():
            @pl.when((y == LINE - 1) & has_prev)
            def _():
                arrived(3, c)

            send_all(pass_sends, c)

            @pl.when(z + 3 < depth)
            def _():
                arrived(2, c)

            send_all(third_sends, c)

        @pl.when(has_0)
        def _():
            @pl.when(z + 1 < depth)
            def _():
                arrived(0, c_0)

            send_all(first_sends, c_0)

        @pl.when((c_1 >= 0) & (z + 2 < depth))
        def _():
            arrived(1, c_1)

        steady = (c_1 >= 0) & (c < CHUNKS)

        @pl.when(steady)
        def _():
            correlate([(2, c), (0, c_0), (1, c_1)])

        @pl.when(jnp.logical_not(steady) & (c < CHUNKS))
        def _():
            correlate([(2, c)])

        @pl.when(jnp.logical_not(steady) & has_0)
        def _():
            correlate([(0, c_0)])

        @pl.when(jnp.logical_not(steady) & (c_1 >= 0))
        def _():
            correlate([(1, c_1)])

        return carry

    lax.fori_loop(0, CHUNKS + LAG, step, 0)

    for k in range(1, 4):
        sums = taps[k - 1]
        weight = weight_t[2 * (k - 1) : 2 * k, 0:columns]
        for a in range(2):
            slope = sums[4 * a : 4 * a + 2, 0:columns]
            size = sums[4 * a + 2 : 4 * a + 4, 0:columns]
            shift = offsets_v[2 * (k - 1) + a].astype(F32)
            value = shift + slope / jnp.maximum(size, floor_ratio * length)
            targets[2 * (k - 1) + a] = value
            target_t[k - 1, 2 * a : 2 * a + 2, 0:columns] = weight * value
    for k in range(1, 4):

        @pl.when(z + k < depth)
        def _():
            t_copy(k).start()

    nodes_rows, nodes_cols = start.shape[1], start.shape[2]
    spread = (
        lax.broadcasted_iota(jnp.int32, (length, nodes_cols), 0)
        == lax.shift_right_logical(lax.broadcasted_iota(jnp.int32, (length, nodes_cols), 1), 4)
    ).astype(F32)

    def widen(small):
        return jnp.dot(small, spread, precision=lax.Precision.HIGHEST, preferred_element_type=F32)

    def tall(wide, first):
        return jnp.concatenate(
            [jnp.broadcast_to(wide[first + r : first + r + 1], (SUB, nodes_cols)) for r in range(rows_dev)], axis=0
        )

    wide_own = widen(weight_t[...])
    for k in range(1, 4):

        @pl.when(z - k >= 0)
        def _():
            w_copy(k).wait_recv()

        weights[k - 1] = tall(wide_own, 2 * (k - 1))
        weights[2 + k] = tall(widen(weight_l[k - 1]), 2 * (k - 1))

    node_row = lax.broadcasted_iota(jnp.int32, (nodes_rows, nodes_cols), 0)
    node_col = lax.broadcasted_iota(jnp.int32, (nodes_rows, nodes_cols), 1)

    def linear(r, value):
        result = []
        for a in range(2):
            u = value[a]
            upper = jnp.where(t == 0, u[0:1], recv_e[r, 0, a : a + 1])
            lower = jnp.where(t == tiles - 1, u[-1:], recv_e[r, 1, a : a + 1])
            up = jnp.where(node_row == 0, upper, pltpu.roll(u, 1, 0))
            down = jnp.where(node_row == nodes_rows - 1, lower, pltpu.roll(u, nodes_rows - 1, 0))
            west = jnp.where(node_col == 0, u, pltpu.roll(u, 1, 1))
            east = jnp.where(node_col == nodes_cols - 1, u, pltpu.roll(u, nodes_cols - 1, 1))
            force = lattice_stiff * (up + down + west + east - 4.0 * u)
            for k in range(1, 4):
                force = force + weights[k - 1] * (recv_z[r, k - 1, a].astype(F32) - u)
                force = force - weights[2 + k] * (u - recv_z[r, 2 + k, a].astype(F32))
            result.append(force)
        return result

    exchange_wait(0)
    base = linear(0, start_value)

    for k in range(1, 4):

        @pl.when(z - k >= 0)
        def _():
            t_copy(k).wait_recv()

    pull = target_l[0] + target_l[1] + target_l[2] - target_t[0] - target_t[1] - target_t[2]
    wide_pull = widen(pull)
    value = [base[a] + tall(wide_pull, 2 * a) for a in range(2)]
    for i in range(ITERS):
        for a in range(2):
            fields[i, a] = value[a]
        if i < ITERS - 1:
            stage(i + 1, value)
            exchange_start(i + 1)
        for n, (first, second) in enumerate(PAIRS):
            if second == i:
                product = fields[first, 0] * value[0] + fields[first, 1] * value[1]
                row = jnp.sum(product, axis=0, keepdims=True)
                gram[n : n + 1] = row[:, :length] + row[:, length:]
        if i < ITERS - 1:
            exchange_wait(i + 1)
            moved = linear(i + 1, value)
            value = [value[a] + step_size * moved[a] for a in range(2)]

    def group_copy(i):
        other = lax.rem(me + i, group)
        return remote(
            gram_row.at[0],
            gram_a.at[me],
            gs.at[0, i],
            gr.at[0, i],
            line * LINE + lax.div(other, tiles),
            lax.rem(other, tiles),
        )

    def lines_copy(i):
        other = lax.rem(line + i, lines)
        return remote(gram_row.at[1], gram_b.at[line], gs.at[1, i], gr.at[1, i], other * LINE + y, t)

    def run(copy, number, what):
        def body(i, carry):
            getattr(copy(i), what)()
            return carry

        lax.fori_loop(1, number, body, 0)

    for n in range(len(PAIRS), gram.shape[0]):
        gram[n : n + 1] = jnp.zeros((1, length), F32)
    summed = jnp.sum(gram[...], axis=1, keepdims=True)
    on_row = lax.broadcasted_iota(jnp.int32, gram.shape, 0) == lax.broadcasted_iota(jnp.int32, gram.shape, 1)
    mine = jnp.sum(jnp.where(on_row, summed, 0.0), axis=0, keepdims=True)
    gram_row[0] = mine
    run(group_copy, group, "start")
    gram_a[me] = mine
    run(group_copy, group, "wait")
    total = gram_a[0]
    for i in range(1, group):
        total = total + gram_a[i]
    gram_row[1] = total
    run(lines_copy, lines, "start")
    gram_b[line] = total
    run(lines_copy, lines, "wait")
    total = gram_b[0]
    for i in range(1, lines):
        total = total + gram_b[i]
    gram_out[...] = jnp.broadcast_to(jnp.sum(jnp.where(on_row, total, 0.0), axis=1, keepdims=True), gram.shape)

    for k in range(1, 4):

        @pl.when(z + k < depth)
        def _():
            w_copy(k).wait_send()
            t_copy(k).wait_send()

    for r in range(ITERS):
        exchange_drain(r)
    for condition, src, dst, send, slot, gz in all_sends:

        @pl.when(condition)
        def _():
            remote(src, dst, ps.at[send], pr.at[slot, 0], gz, t).wait_send()

    pltpu.make_async_copy(staged, surfaces, surf_sem).wait()


def finish(number, start_h, fields_h, gram_h, targets_h, staged, positions, targets, surfaces, norms, held, start, fields, gram, sem_in, sem_out, sem):
    ways = [
        pltpu.make_async_copy(source, to, sem.at[n])
        for n, (source, to) in enumerate(((gram_h, gram), (start_h, start), (fields_h, fields), (targets_h, targets)))
    ]
    for copy in ways:
        copy.start()
    pieces = held.shape[0] // 4
    inward, outward = [], []
    for n in range(4):
        part = pl.ds(n * pieces, pieces)
        inward.append(pltpu.make_async_copy(staged.at[part], held.at[part], sem_in.at[n]))
        outward.append(pltpu.make_async_copy(held.at[part], surfaces.at[part], sem_out.at[n]))
        inward[n].start()
    for copy in ways:
        copy.wait()
    for n in range(4):
        inward[n].wait()
        outward[n].start()
    length = gram.shape[1]
    total = gram[...]

    entries = {}
    for n, (first, second) in enumerate(PAIRS):
        entries[first, second] = entries[second, first] = total[n : n + 1]
    ones = jnp.ones((1, length), F32)
    coefficients = [ones]
    sums = [jnp.zeros((1, length), F32)] * ITERS
    for i in range(ITERS):
        square = jnp.zeros((1, length), F32)
        for first in range(len(coefficients)):
            for second in range(len(coefficients)):
                square = square + coefficients[first] * coefficients[second] * entries[first, second]
        rms = jnp.sqrt(jnp.maximum(square, 0.0) / number + tiny_eps)
        norms[i] = rms[0, 0]
        factor = jnp.minimum(1.0, clip_level / rms)
        for n in range(len(coefficients)):
            sums[n] = sums[n] + step_size * factor * coefficients[n]
        kept = [(1.0 - factor) * value for value in coefficients] + [0.0 * ones]
        shifted = [0.0 * ones] + [factor * value for value in coefficients]
        coefficients = [kept[n] + shifted[n] for n in range(len(shifted))]
    for a in range(2):
        result = start[a]
        for n in range(ITERS):
            result = result + jnp.concatenate([sums[n], sums[n]], axis=1) * fields[n, a]
        positions[a] = result
    for copy in outward:
        copy.wait()


def local(depth, tiles, patches, peak_offsets, valid_masks, initial_positions):
    _, rows_dev, columns, length, _ = patches.shape
    count = rows_dev * columns
    _, _, nodes_rows, nodes_cols = initial_positions.shape
    offsets = peak_offsets.reshape(6, rows_dev, columns)
    vmem = pl.BlockSpec(memory_space=pltpu.VMEM)
    smem = pl.BlockSpec(memory_space=pltpu.SMEM)
    hbm = pl.BlockSpec(memory_space=pltpu.HBM)
    group = LINE * tiles
    lines = depth // LINE
    dma = pltpu.SemaphoreType.DMA
    flops = 2 * count * (4 * 6 + 3 * 6) * length**3
    start = initial_positions.reshape(2, nodes_rows, nodes_cols)
    targets, staged, fields, gram = pl.pallas_call(
        functools.partial(kernel, depth, tiles),
        out_shape=(
            jax.ShapeDtypeStruct((6, rows_dev, columns), F32),
            jax.ShapeDtypeStruct((3, count, length, length), BF16),
            jax.ShapeDtypeStruct((ITERS, 2, nodes_rows, nodes_cols), F32),
            jax.ShapeDtypeStruct((16, length), F32),
        ),
        in_specs=[hbm, hbm, hbm, hbm, hbm],
        out_specs=(vmem, hbm, vmem, vmem),
        scratch_shapes=[
            pltpu.VMEM((count, length, length), BF16),
            pltpu.VMEM((3, count, length, length), BF16),
            pltpu.VMEM((count, length, length), BF16),
            pltpu.VMEM((count, length, length), F32),
            pltpu.VMEM((count, length, length), F32),
            pltpu.VMEM((3, count, length, length), BF16),
            pltpu.SMEM((6, rows_dev, columns), jnp.int32),
            pltpu.VMEM((6, rows_dev, columns), jnp.int32),
            pltpu.VMEM((3, rows_dev, columns), jnp.int32),
            pltpu.VMEM((2, nodes_rows, nodes_cols), F32),
            pltpu.VMEM((6 * length, 2 * length), BF16),
            pltpu.VMEM((3, 8, length), F32),
            pltpu.VMEM((ITERS, 2, nodes_rows, nodes_cols), BF16),
            pltpu.VMEM((ITERS, 6, 2, nodes_rows, nodes_cols), BF16),
            pltpu.VMEM((ITERS, 2, 8, nodes_cols), F32),
            pltpu.VMEM((ITERS, 2, 8, nodes_cols), F32),
            pltpu.VMEM((8, length), F32),
            pltpu.VMEM((3, 8, length), F32),
            pltpu.VMEM((3, 8, length), F32),
            pltpu.VMEM((3, 8, length), F32),
            pltpu.VMEM((6, nodes_rows, nodes_cols), F32),
            pltpu.VMEM((16, length), F32),
            pltpu.VMEM((2, 1, length), F32),
            pltpu.VMEM((group, 1, length), F32),
            pltpu.VMEM((lines, 1, length), F32),
            dma((CHUNKS,)),
            dma((5,)),
            dma,
            dma((6,)),
            dma((4, CHUNKS)),
            dma((ITERS, 6)),
            dma((ITERS, 6)),
            dma((ITERS, 2)),
            dma((ITERS, 2)),
            dma((3,)),
            dma((3,)),
            dma((3,)),
            dma((3,)),
            dma((2, max(group, lines))),
            dma((2, max(group, lines))),
        ],
        compiler_params=pltpu.CompilerParams(collective_id=0, has_side_effects=True),
        cost_estimate=pl.CostEstimate(flops=flops, bytes_accessed=5 * count * length * length * 2, transcendentals=0),
    )(
        patches.reshape(count, length, length),
        offsets,
        valid_masks.reshape(3, rows_dev, columns),
        start,
        jnp.asarray(tables(length)),
    )
    number = 2.0 * depth * tiles * nodes_rows * nodes_cols
    positions, targets, surfaces, norms = pl.pallas_call(
        functools.partial(finish, number),
        out_shape=(
            jax.ShapeDtypeStruct((2, nodes_rows, nodes_cols), F32),
            jax.ShapeDtypeStruct((6, rows_dev, columns), F32),
            jax.ShapeDtypeStruct((3 * count, length, length), BF16),
            jax.ShapeDtypeStruct((ITERS,), F32),
        ),
        in_specs=[hbm, hbm, hbm, hbm, hbm],
        out_specs=(vmem, vmem, hbm, smem),
        scratch_shapes=[
            pltpu.VMEM((3 * count, length, length), BF16),
            pltpu.VMEM((2, nodes_rows, nodes_cols), F32),
            pltpu.VMEM((ITERS, 2, nodes_rows, nodes_cols), F32),
            pltpu.VMEM((16, length), F32),
            dma((4,)),
            dma((4,)),
            dma((4,)),
        ],
    )(start, fields, gram, targets, staged.reshape(3 * count, length, length))
    return (
        positions.reshape(initial_positions.shape),
        targets.reshape(peak_offsets.shape),
        surfaces.reshape(1, 3, rows_dev, columns, length, length),
        norms,
    )


def solution(mesh):
    depth, tiles = mesh.shape["gz"], mesh.shape["xy"]
    placed = (
        P("gz", "xy", None, None, None),
        P("gz", None, "xy", None),
        P("gz", None, "xy", None),
        P(None, "gz", "xy", None),
    )
    return jax.shard_map(
        functools.partial(local, depth, tiles),
        mesh=mesh,
        in_specs=placed,
        out_specs=(
            P(None, "gz", "xy", None),
            P("gz", None, "xy", None),
            P("gz", None, "xy", None, None, None),
            P(),
        ),
        check_vma=False,
    )
```

```python
import functools

import numpy as np

import jax
import jax.numpy as jnp
from jax import lax
from jax.experimental import pallas as pl
from jax.experimental.pallas import tpu as pltpu
from jax.sharding import PartitionSpec as P

SUB = 16
ITERS = 4
LINE = 4
CHUNKS = 16
AHEAD = 8
FAR_AHEAD = 3
OWN_STEP = 8
LAG = 2

lattice_stiff = 0.5
clip_level = 5.0
step_size = 0.2
floor_ratio = 0.4
tiny_eps = 1e-06

MESH = pl.DeviceIdType.MESH
F32 = jnp.float32
BF16 = jnp.bfloat16
PAIRS = [(i, j) for i in range(ITERS) for j in range(i, ITERS)]


def tables(length):
    series = np.arange(length)
    angles = 2.0 * np.pi / length * (series[:, None] * series[None, :] % length)
    cosine = np.cos(angles).astype(jnp.bfloat16)
    sine = np.sin(angles).astype(jnp.bfloat16)
    right = np.concatenate([cosine, sine], axis=1)
    left = np.block([[cosine, -sine], [-sine, -cosine]])
    back = np.block([[cosine, sine], [-sine, cosine]])
    last = np.concatenate([cosine, -sine], axis=1)
    return np.concatenate([right, left, back, last], axis=0)


def kernel(
    depth,
    tiles,
    patches,
    offsets_h,
    masks_h,
    start_h,
    tables_h,
    targets,
    surfaces,
    fields,
    gram_out,
    own,
    near,
    passing,
    spec_real,
    spec_imag,
    staged,
    offsets,
    offsets_v,
    masks,
    start,
    table,
    taps,
    send_z,
    recv_z,
    send_e,
    recv_e,
    weight_t,
    weight_l,
    target_t,
    target_l,
    weights,
    gram,
    gram_row,
    gram_a,
    gram_b,
    local_sem,
    in_sem,
    surf_sem,
    ps,
    pr,
    zs,
    zr,
    es,
    er,
    ws,
    wr,
    ts,
    tr,
    gs,
    gr,
):
    z = lax.axis_index("gz")
    t = lax.axis_index("xy")
    count, length, _ = own.shape
    piece = count // CHUNKS
    columns = masks_h.shape[2]
    rows_dev = masks_h.shape[1]
    lines = depth // LINE
    y = lax.rem(z, LINE)
    line = lax.div(z, LINE)
    has_next = line < lines - 1
    has_prev = line > 0
    group = LINE * tiles
    me = y * tiles + t

    def remote(src, dst, send, recv, gz, xy):
        return pltpu.make_async_remote_copy(
            src_ref=src, dst_ref=dst, send_sem=send, recv_sem=recv, device_id=(gz, xy), device_id_type=MESH
        )

    def local_copy(c):
        part = pl.ds(c * piece, piece)
        return pltpu.make_async_copy(patches.at[part], own.at[part], local_sem.at[c])

    inputs = [
        pltpu.make_async_copy(source, held, in_sem.at[n])
        for n, (source, held) in enumerate(
            ((masks_h, masks), (start_h, start), (offsets_h, offsets_v), (offsets_h, offsets), (tables_h, table))
        )
    ]
    for copy in inputs:
        copy.start()
    right = table.at[0:length]
    left = table.at[length : 3 * length]
    back = table.at[3 * length : 5 * length]
    last = table.at[5 * length : 6 * length]

    def start_local(c, carry):
        local_copy(c).start()
        return carry

    lax.fori_loop(0, CHUNKS, start_local, 0)

    barrier = pltpu.get_barrier_semaphore()

    def greet_group(i, carry):
        other = lax.rem(me + i, group)
        gz = line * LINE + lax.div(other, tiles)
        pl.semaphore_signal(barrier, inc=1, device_id=(gz, lax.rem(other, tiles)), device_id_type=MESH)
        return carry

    lax.fori_loop(1, group, greet_group, 0)

    def greet_lines(i, carry):
        other = lax.rem(line + i, lines)
        pl.semaphore_signal(barrier, inc=1, device_id=(other * LINE + y, t), device_id_type=MESH)
        return carry

    lax.fori_loop(1, lines, greet_lines, 0)
    for k in range(1, 4):
        for sign in (-1, 1):
            there = z + sign * k

            @pl.when((there >= 0) & (there < depth))
            def _():
                pl.semaphore_signal(barrier, inc=1, device_id=(there, t), device_id_type=MESH)

    for k in range(1, 4):

        @pl.when(z + k >= depth)
        def _():
            near[k - 1] = jnp.zeros(near.shape[1:], BF16)
            for r in range(ITERS):
                recv_z[r, k - 1] = jnp.zeros(recv_z.shape[2:], BF16)

        @pl.when(z - k < 0)
        def _():
            for r in range(ITERS):
                recv_z[r, 2 + k] = jnp.zeros(recv_z.shape[2:], BF16)
            weight_l[k - 1] = jnp.zeros(weight_l.shape[1:], F32)
            target_l[k - 1] = jnp.zeros(target_l.shape[1:], F32)

    inputs[0].wait()
    inputs[1].wait()
    weight_t[...] = jnp.zeros(weight_t.shape, F32)
    target_t[...] = jnp.zeros(target_t.shape, F32)
    taps[...] = jnp.zeros(taps.shape, F32)
    for k in range(1, 4):
        live = jnp.where(z + k < depth, 1.0 / k, 0.0).astype(F32)
        weight_t[2 * (k - 1) : 2 * k, 0:columns] = masks[k - 1].astype(F32) * live

    def stage(r, value):
        for a in range(2):
            send_z[r, a] = value[a].astype(BF16)
            send_e[r, 0, a : a + 1] = value[a][0:1]
            send_e[r, 1, a : a + 1] = value[a][-1:]

    start_value = [start[0], start[1]]
    stage(0, start_value)

    for copy in inputs[2:]:
        copy.wait()
    half = length

    def dot(a, b):
        return jnp.dot(a, b, preferred_element_type=F32)

    def side_by_side(m):
        return jnp.concatenate(
            [
                jnp.concatenate([m[:half, :half], m[half:, :half]], axis=1),
                jnp.concatenate([m[:half, half:], m[half:, half:]], axis=1),
            ],
            axis=0,
        )

    def spectra(sources):
        mixed = [dot(ref[pl.ds(p, 2)].reshape(2 * half, half), right[...]).astype(BF16) for ref, p in sources]
        return [dot(left[...], side_by_side(m)) for m in mixed]

    def own_spectra(i, carry):
        firsts = [OWN_STEP * i + 2 * n for n in range(OWN_STEP // 2)]
        for p, s in zip(firsts, spectra([(own, p) for p in firsts])):
            for a in range(2):
                cols = slice(a * half, (a + 1) * half)
                spec_real[p + a] = s[:half, cols]
                spec_imag[p + a] = s[half:, cols]
        return carry

    def wait_local(c, carry):
        local_copy(c).wait()
        return carry

    lax.fori_loop(0, CHUNKS, wait_local, 0)
    lax.fori_loop(0, count // OWN_STEP, own_spectra, 0)

    expected = group - 1 + lines - 1
    for k in range(1, 4):
        expected = expected + (z + k < depth).astype(jnp.int32) + (z - k >= 0).astype(jnp.int32)
    pl.semaphore_wait(barrier, expected)

    def z_copy(r, k, sign):
        slot = 2 + k if sign > 0 else k - 1
        return remote(send_z.at[r], recv_z.at[r, slot], zs.at[r, slot], zr.at[r, slot], z + sign * k, t)

    def e_copy(r, sign):
        side = 1 if sign > 0 else 0
        return remote(send_e.at[r, side], recv_e.at[r, 1 - side], es.at[r, side], er.at[r, 1 - side], z, t + sign)

    def exchange_start(r):
        for k in (3, 2, 1):
            for sign in (-1, 1):

                @pl.when((z + sign * k >= 0) & (z + sign * k < depth))
                def _():
                    z_copy(r, k, sign).start()

        for sign in (-1, 1):

            @pl.when((t + sign >= 0) & (t + sign < tiles))
            def _():
                e_copy(r, sign).start()

    def exchange_wait(r):
        for k in (1, 2, 3):
            for sign in (-1, 1):

                @pl.when((z - sign * k >= 0) & (z - sign * k < depth))
                def _():
                    z_copy(r, k, sign).wait_recv()

        for sign in (-1, 1):

            @pl.when((t - sign >= 0) & (t - sign < tiles))
            def _():
                e_copy(r, sign).wait_recv()

    def exchange_drain(r):
        for k in (1, 2, 3):
            for sign in (-1, 1):

                @pl.when((z + sign * k >= 0) & (z + sign * k < depth))
                def _():
                    z_copy(r, k, sign).wait_send()

        for sign in (-1, 1):

            @pl.when((t + sign >= 0) & (t + sign < tiles))
            def _():
                e_copy(r, sign).wait_send()

    def w_copy(k):
        return remote(weight_t, weight_l.at[k - 1], ws.at[k - 1], wr.at[k - 1], z + k, t)

    def t_copy(k):
        return remote(target_t.at[k - 1], target_l.at[k - 1], ts.at[k - 1], tr.at[k - 1], z + k, t)

    def part_of(c):
        return pl.ds(c * piece, piece)

    def patch_copy(src, dst, send, slot, c, gz):
        part = part_of(c)
        return remote(src.at[part], dst.at[part], ps.at[send], pr.at[slot, c], gz, t)

    relays = (y == 1) | (y == 2)
    far_sends = [
        (z >= 3, own, near.at[2], 0, 2, z - 3),
        ((y == 0) & has_prev, own, passing, 2, 3, z + 3),
    ]
    next_sends = [(y >= 1, own, near.at[0], 1, 0, z - 1)]
    pass_sends = [((y == LINE - 1) & has_prev, passing, near.at[0], 3, 0, z - LINE)]
    first_sends = [(relays, near.at[0], near.at[1], 4, 1, z - 1)]
    third_sends = [(relays & has_next, near.at[2], near.at[1], 5, 1, z + 1)]
    all_sends = far_sends + next_sends + pass_sends + first_sends + third_sends

    def send_all(sends, c):
        for condition, src, dst, send, slot, gz in sends:

            @pl.when(condition)
            def _():
                patch_copy(src, dst, send, slot, c, gz).start()

    def arrived(slot, c):
        buffer = passing if slot == 3 else near.at[slot]
        patch_copy(buffer, buffer, 0, slot, c, z).wait_recv()

    for k in range(1, 4):

        @pl.when(z + k < depth)
        def _():
            w_copy(k).start()

    def send_far(c, carry):
        send_all(far_sends, c)
        return carry

    def send_next(c, carry):
        send_all(next_sends, c)
        return carry

    lax.fori_loop(0, AHEAD, send_next, 0)
    lax.fori_loop(0, FAR_AHEAD, send_far, 0)

    row_id = lax.broadcasted_iota(jnp.int32, (16, length), 0)
    row_id = jnp.where(row_id < 8, row_id, row_id - 16)
    col_id = lax.broadcasted_iota(jnp.int32, (16, length), 1)
    col_id = jnp.where(col_id < length // 2, col_id, col_id - length)
    tap_row = lax.broadcasted_iota(jnp.int32, (8, length), 0)
    tap_col = lax.broadcasted_iota(jnp.int32, (8, length), 1)

    def pick(k, p, window):
        r = lax.div(p, columns)
        c = lax.rem(p, columns)
        d_row = row_id - offsets[2 * k, r, c]
        d_col = col_id - offsets[2 * k + 1, r, c]
        down = jnp.where((d_col == 0) & (jnp.abs(d_row) <= 1), window, 0.0)
        across = jnp.where((d_row == 0) & (jnp.abs(d_col) <= 1), window, 0.0)

        def total(v):
            return jnp.sum(jnp.sum(v, axis=0, keepdims=True), axis=1, keepdims=True)

        sums = (
            total(down * d_row.astype(F32)),
            total(jnp.abs(down)),
            total(across * d_col.astype(F32)),
            total(jnp.abs(across)),
        )
        value = taps[k]
        for q in range(4):
            value = jnp.where((tap_row == 2 * q + r) & (tap_col == c), sums[q], value)
        taps[k] = value

    def correlate(works):
        pairs = [(k, c * piece + 2 * i) for i in range(piece // 2) for k, c in works]
        crossed = []
        for (k, p), s in zip(pairs, spectra([(near.at[k], p) for k, p in pairs])):
            mixed = []
            for a in range(2):
                cols = slice(a * half, (a + 1) * half)
                b_real, b_imag = s[:half, cols], s[half:, cols]
                a_real, a_imag = spec_real[p + a], spec_imag[p + a]
                real = (a_real * b_real + a_imag * b_imag).astype(BF16)
                imag = (a_real * b_imag - a_imag * b_real).astype(BF16)
                mixed.append(jnp.concatenate([real, imag], axis=1))
            crossed.append(jnp.concatenate(mixed, axis=0))
        halves = [dot(m, back[...]).astype(BF16) for m in crossed]
        corrs = [dot(last[...], side_by_side(h)) * (1.0 / (length * length)) for h in halves]
        for (k, p), corr in zip(pairs, corrs):
            for a in range(2):
                one = corr[:, a * half : (a + 1) * half]
                staged[k, p + a] = one.astype(BF16)
                pick(k, p + a, jnp.concatenate([one[:8], one[length - 8 :]], axis=0))
        for k, c in works:
            part = part_of(c)
            pltpu.make_async_copy(staged.at[k, part], surfaces.at[k, part], surf_sem).start()

    late = jnp.where(y == LINE - 1, LAG, 0)

    def step(c, carry):
        @pl.when(c < CHUNKS - FAR_AHEAD)
        def _():
            send_far(c + FAR_AHEAD, 0)

        @pl.when(c < CHUNKS - AHEAD)
        def _():
            send_next(c + AHEAD, 0)

        @pl.when(c == CHUNKS)
        def _():
            exchange_start(0)

        c_0 = c - late
        c_1 = c - LAG
        has_0 = (c_0 >= 0) & (c_0 < CHUNKS)

        @pl.when(c < CHUNKS)
        def _():
            @pl.when((y == LINE - 1) & has_prev)
            def _():
                arrived(3, c)

            send_all(pass_sends, c)

            @pl.when(z + 3 < depth)
            def _():
                arrived(2, c)

            send_all(third_sends, c)

        @pl.when(has_0)
        def _():
            @pl.when(z + 1 < depth)
            def _():
                arrived(0, c_0)

            send_all(first_sends, c_0)

        @pl.when((c_1 >= 0) & (z + 2 < depth))
        def _():
            arrived(1, c_1)

        steady = (c_1 >= 0) & (c < CHUNKS)

        @pl.when(steady)
        def _():
            correlate([(2, c), (0, c_0), (1, c_1)])

        @pl.when(jnp.logical_not(steady) & (c < CHUNKS))
        def _():
            correlate([(2, c)])

        @pl.when(jnp.logical_not(steady) & has_0)
        def _():
            correlate([(0, c_0)])

        @pl.when(jnp.logical_not(steady) & (c_1 >= 0))
        def _():
            correlate([(1, c_1)])

        return carry

    lax.fori_loop(0, CHUNKS + LAG, step, 0)

    for k in range(1, 4):
        sums = taps[k - 1]
        weight = weight_t[2 * (k - 1) : 2 * k, 0:columns]
        for a in range(2):
            slope = sums[4 * a : 4 * a + 2, 0:columns]
            size = sums[4 * a + 2 : 4 * a + 4, 0:columns]
            shift = offsets_v[2 * (k - 1) + a].astype(F32)
            value = shift + slope / jnp.maximum(size, floor_ratio * length)
            targets[2 * (k - 1) + a] = value
            target_t[k - 1, 2 * a : 2 * a + 2, 0:columns] = weight * value
    for k in range(1, 4):

        @pl.when(z + k < depth)
        def _():
            t_copy(k).start()

    nodes_rows, nodes_cols = start.shape[1], start.shape[2]
    spread = (
        lax.broadcasted_iota(jnp.int32, (length, nodes_cols), 0)
        == lax.shift_right_logical(lax.broadcasted_iota(jnp.int32, (length, nodes_cols), 1), 4)
    ).astype(F32)

    def widen(small):
        return jnp.dot(small, spread, precision=lax.Precision.HIGHEST, preferred_element_type=F32)

    def tall(wide, first):
        return jnp.concatenate(
            [jnp.broadcast_to(wide[first + r : first + r + 1], (SUB, nodes_cols)) for r in range(rows_dev)], axis=0
        )

    wide_own = widen(weight_t[...])
    for k in range(1, 4):

        @pl.when(z - k >= 0)
        def _():
            w_copy(k).wait_recv()

        weights[k - 1] = tall(wide_own, 2 * (k - 1))
        weights[2 + k] = tall(widen(weight_l[k - 1]), 2 * (k - 1))

    node_row = lax.broadcasted_iota(jnp.int32, (nodes_rows, nodes_cols), 0)
    node_col = lax.broadcasted_iota(jnp.int32, (nodes_rows, nodes_cols), 1)

    def linear(r, value):
        result = []
        for a in range(2):
            u = value[a]
            upper = jnp.where(t == 0, u[0:1], recv_e[r, 0, a : a + 1])
            lower = jnp.where(t == tiles - 1, u[-1:], recv_e[r, 1, a : a + 1])
            up = jnp.where(node_row == 0, upper, pltpu.roll(u, 1, 0))
            down = jnp.where(node_row == nodes_rows - 1, lower, pltpu.roll(u, nodes_rows - 1, 0))
            west = jnp.where(node_col == 0, u, pltpu.roll(u, 1, 1))
            east = jnp.where(node_col == nodes_cols - 1, u, pltpu.roll(u, nodes_cols - 1, 1))
            force = lattice_stiff * (up + down + west + east - 4.0 * u)
            for k in range(1, 4):
                force = force + weights[k - 1] * (recv_z[r, k - 1, a].astype(F32) - u)
                force = force - weights[2 + k] * (u - recv_z[r, 2 + k, a].astype(F32))
            result.append(force)
        return result

    exchange_wait(0)
    base = linear(0, start_value)

    for k in range(1, 4):

        @pl.when(z - k >= 0)
        def _():
            t_copy(k).wait_recv()

    pull = target_l[0] + target_l[1] + target_l[2] - target_t[0] - target_t[1] - target_t[2]
    wide_pull = widen(pull)
    value = [base[a] + tall(wide_pull, 2 * a) for a in range(2)]
    for i in range(ITERS):
        for a in range(2):
            fields[i, a] = value[a]
        if i < ITERS - 1:
            stage(i + 1, value)
            exchange_start(i + 1)
        for n, (first, second) in enumerate(PAIRS):
            if second == i:
                product = fields[first, 0] * value[0] + fields[first, 1] * value[1]
                row = jnp.sum(product, axis=0, keepdims=True)
                gram[n : n + 1] = row[:, :length] + row[:, length:]
        if i < ITERS - 1:
            exchange_wait(i + 1)
            moved = linear(i + 1, value)
            value = [value[a] + step_size * moved[a] for a in range(2)]

    def group_copy(i):
        other = lax.rem(me + i, group)
        return remote(
            gram_row.at[0],
            gram_a.at[me],
            gs.at[0, i],
            gr.at[0, i],
            line * LINE + lax.div(other, tiles),
            lax.rem(other, tiles),
        )

    def lines_copy(i):
        other = lax.rem(line + i, lines)
        return remote(gram_row.at[1], gram_b.at[line], gs.at[1, i], gr.at[1, i], other * LINE + y, t)

    def run(copy, number, what):
        def body(i, carry):
            getattr(copy(i), what)()
            return carry

        lax.fori_loop(1, number, body, 0)

    for n in range(len(PAIRS), gram.shape[0]):
        gram[n : n + 1] = jnp.zeros((1, length), F32)
    summed = jnp.sum(gram[...], axis=1, keepdims=True)
    on_row = lax.broadcasted_iota(jnp.int32, gram.shape, 0) == lax.broadcasted_iota(jnp.int32, gram.shape, 1)
    mine = jnp.sum(jnp.where(on_row, summed, 0.0), axis=0, keepdims=True)
    gram_row[0] = mine
    run(group_copy, group, "start")
    gram_a[me] = mine
    run(group_copy, group, "wait")
    total = gram_a[0]
    for i in range(1, group):
        total = total + gram_a[i]
    gram_row[1] = total
    run(lines_copy, lines, "start")
    gram_b[line] = total
    run(lines_copy, lines, "wait")
    total = gram_b[0]
    for i in range(1, lines):
        total = total + gram_b[i]
    gram_out[...] = jnp.broadcast_to(jnp.sum(jnp.where(on_row, total, 0.0), axis=1, keepdims=True), gram.shape)

    for k in range(1, 4):

        @pl.when(z + k < depth)
        def _():
            w_copy(k).wait_send()
            t_copy(k).wait_send()

    for r in range(ITERS):
        exchange_drain(r)
    for condition, src, dst, send, slot, gz in all_sends:

        @pl.when(condition)
        def _():
            remote(src, dst, ps.at[send], pr.at[slot, 0], gz, t).wait_send()

    pltpu.make_async_copy(staged, surfaces, surf_sem).wait()


def finish(number, start_h, fields_h, gram_h, targets_h, staged, positions, targets, surfaces, norms, held, start, fields, gram, sem_in, sem_out, sem):
    ways = [
        pltpu.make_async_copy(source, to, sem.at[n])
        for n, (source, to) in enumerate(((gram_h, gram), (start_h, start), (fields_h, fields), (targets_h, targets)))
    ]
    for copy in ways:
        copy.start()
    pieces = held.shape[0] // 4
    inward, outward = [], []
    for n in range(4):
        part = pl.ds(n * pieces, pieces)
        inward.append(pltpu.make_async_copy(staged.at[part], held.at[part], sem_in.at[n]))
        outward.append(pltpu.make_async_copy(held.at[part], surfaces.at[part], sem_out.at[n]))
        inward[n].start()
    for copy in ways:
        copy.wait()
    for n in range(4):
        inward[n].wait()
        outward[n].start()
    length = gram.shape[1]
    total = gram[...]

    entries = {}
    for n, (first, second) in enumerate(PAIRS):
        entries[first, second] = entries[second, first] = total[n : n + 1]
    ones = jnp.ones((1, length), F32)
    coefficients = [ones]
    sums = [jnp.zeros((1, length), F32)] * ITERS
    for i in range(ITERS):
        square = jnp.zeros((1, length), F32)
        for first in range(len(coefficients)):
            for second in range(len(coefficients)):
                square = square + coefficients[first] * coefficients[second] * entries[first, second]
        rms = jnp.sqrt(jnp.maximum(square, 0.0) / number + tiny_eps)
        norms[i] = rms[0, 0]
        factor = jnp.minimum(1.0, clip_level / rms)
        for n in range(len(coefficients)):
            sums[n] = sums[n] + step_size * factor * coefficients[n]
        kept = [(1.0 - factor) * value for value in coefficients] + [0.0 * ones]
        shifted = [0.0 * ones] + [factor * value for value in coefficients]
        coefficients = [kept[n] + shifted[n] for n in range(len(shifted))]
    for a in range(2):
        result = start[a]
        for n in range(ITERS):
            result = result + jnp.concatenate([sums[n], sums[n]], axis=1) * fields[n, a]
        positions[a] = result
    for copy in outward:
        copy.wait()


def local(depth, tiles, patches, peak_offsets, valid_masks, initial_positions):
    _, rows_dev, columns, length, _ = patches.shape
    count = rows_dev * columns
    _, _, nodes_rows, nodes_cols = initial_positions.shape
    offsets = peak_offsets.reshape(6, rows_dev, columns)
    vmem = pl.BlockSpec(memory_space=pltpu.VMEM)
    smem = pl.BlockSpec(memory_space=pltpu.SMEM)
    hbm = pl.BlockSpec(memory_space=pltpu.HBM)
    group = LINE * tiles
    lines = depth // LINE
    dma = pltpu.SemaphoreType.DMA
    flops = 2 * count * (4 * 6 + 3 * 6) * length**3
    start = initial_positions.reshape(2, nodes_rows, nodes_cols)
    targets, staged, fields, gram = pl.pallas_call(
        functools.partial(kernel, depth, tiles),
        out_shape=(
            jax.ShapeDtypeStruct((6, rows_dev, columns), F32),
            jax.ShapeDtypeStruct((3, count, length, length), BF16),
            jax.ShapeDtypeStruct((ITERS, 2, nodes_rows, nodes_cols), F32),
            jax.ShapeDtypeStruct((16, length), F32),
        ),
        in_specs=[hbm, hbm, hbm, hbm, hbm],
        out_specs=(vmem, hbm, vmem, vmem),
        scratch_shapes=[
            pltpu.VMEM((count, length, length), BF16),
            pltpu.VMEM((3, count, length, length), BF16),
            pltpu.VMEM((count, length, length), BF16),
            pltpu.VMEM((count, length, length), F32),
            pltpu.VMEM((count, length, length), F32),
            pltpu.VMEM((3, count, length, length), BF16),
            pltpu.SMEM((6, rows_dev, columns), jnp.int32),
            pltpu.VMEM((6, rows_dev, columns), jnp.int32),
            pltpu.VMEM((3, rows_dev, columns), jnp.int32),
            pltpu.VMEM((2, nodes_rows, nodes_cols), F32),
            pltpu.VMEM((6 * length, 2 * length), BF16),
            pltpu.VMEM((3, 8, length), F32),
            pltpu.VMEM((ITERS, 2, nodes_rows, nodes_cols), BF16),
            pltpu.VMEM((ITERS, 6, 2, nodes_rows, nodes_cols), BF16),
            pltpu.VMEM((ITERS, 2, 8, nodes_cols), F32),
            pltpu.VMEM((ITERS, 2, 8, nodes_cols), F32),
            pltpu.VMEM((8, length), F32),
            pltpu.VMEM((3, 8, length), F32),
            pltpu.VMEM((3, 8, length), F32),
            pltpu.VMEM((3, 8, length), F32),
            pltpu.VMEM((6, nodes_rows, nodes_cols), F32),
            pltpu.VMEM((16, length), F32),
            pltpu.VMEM((2, 1, length), F32),
            pltpu.VMEM((group, 1, length), F32),
            pltpu.VMEM((lines, 1, length), F32),
            dma((CHUNKS,)),
            dma((5,)),
            dma,
            dma((6,)),
            dma((4, CHUNKS)),
            dma((ITERS, 6)),
            dma((ITERS, 6)),
            dma((ITERS, 2)),
            dma((ITERS, 2)),
            dma((3,)),
            dma((3,)),
            dma((3,)),
            dma((3,)),
            dma((2, max(group, lines))),
            dma((2, max(group, lines))),
        ],
        compiler_params=pltpu.CompilerParams(collective_id=0, has_side_effects=True),
        cost_estimate=pl.CostEstimate(flops=flops, bytes_accessed=5 * count * length * length * 2, transcendentals=0),
    )(
        patches.reshape(count, length, length),
        offsets,
        valid_masks.reshape(3, rows_dev, columns),
        start,
        jnp.asarray(tables(length)),
    )
    number = 2.0 * depth * tiles * nodes_rows * nodes_cols
    positions, targets, surfaces, norms = pl.pallas_call(
        functools.partial(finish, number),
        out_shape=(
            jax.ShapeDtypeStruct((2, nodes_rows, nodes_cols), F32),
            jax.ShapeDtypeStruct((6, rows_dev, columns), F32),
            jax.ShapeDtypeStruct((3 * count, length, length), BF16),
            jax.ShapeDtypeStruct((ITERS,), F32),
        ),
        in_specs=[hbm, hbm, hbm, hbm, hbm],
        out_specs=(vmem, vmem, hbm, smem),
        scratch_shapes=[
            pltpu.VMEM((3 * count, length, length), BF16),
            pltpu.VMEM((2, nodes_rows, nodes_cols), F32),
            pltpu.VMEM((ITERS, 2, nodes_rows, nodes_cols), F32),
            pltpu.VMEM((16, length), F32),
            dma((4,)),
            dma((4,)),
            dma((4,)),
        ],
    )(start, fields, gram, targets, staged.reshape(3 * count, length, length))
    return (
        positions.reshape(initial_positions.shape),
        targets.reshape(peak_offsets.shape),
        surfaces.reshape(1, 3, rows_dev, columns, length, length),
        norms,
    )


def solution(mesh):
    depth, tiles = mesh.shape["gz"], mesh.shape["xy"]
    placed = (
        P("gz", "xy", None, None, None),
        P("gz", None, "xy", None),
        P("gz", None, "xy", None),
        P(None, "gz", "xy", None),
    )
    return jax.shard_map(
        functools.partial(local, depth, tiles),
        mesh=mesh,
        in_specs=placed,
        out_specs=(
            P(None, "gz", "xy", None),
            P("gz", None, "xy", None),
            P("gz", None, "xy", None, None, None),
            P(),
        ),
        check_vma=False,
    )
```
